128 devices in a mesh: row: 16 (over y, x_hi, core), col: 8 (over x_lo, z).
Axes of the slice: x: 4 (x_hi: 2, x_lo: 2; x = x_hi * 2 + x_lo), y: 4, z: 4, core: 2. Of those that a mesh axis runs over, the one named last changes fastest.
Arguments:
- image: bfloat16 [768, 512, 256], P('row', 'col'), may hold values from -6 to 6
- norm_gain: float32 [2, 2, 256], replicated, may hold values from 0.1 to 1.9
- conv_first: bfloat16 [2, 3, 3, 256, 256], replicated, may hold values from -0.125 to 0.125
- conv_second: bfloat16 [2, 3, 3, 256, 256], replicated, may hold values from -0.125 to 0.125
- proj_in: bfloat16 [2, 256, 512], replicated, may hold values from -0.375 to 0.375
- block_mix: bfloat16 [2, 256, 256], replicated, may hold values from -0.375 to 0.375
- block_bias: float32 [2, 256], replicated, may hold values from 0.5 to 1.5
- grid_mix: bfloat16 [2, 128, 128], replicated, may hold values from -0.5 to 0.5
- grid_bias: float32 [2, 128], replicated, may hold values from 0.5 to 1.5
- proj_out: bfloat16 [2, 256, 256], replicated, may hold values from -0.375 to 0.375
Outputs:
- restored: bfloat16 [768, 512, 256], P('row', 'col')
The draws below stay inside these ranges and needn't reach their ends.
All inputs are finite; a program needn't handle non-finite values.
Results may differ from the reference program's by a relative error of at most 0.012.
Values may be sent and summed in bfloat16 or wider, within the bound.
A program may use at most 128 MiB of HBM per device.

```python
import jax
import jax.numpy as jnp
from jax import lax

C = 256
BLOCK = 16
LAYERS = 2
CH = 48
CW = 64
POSITIONS = 256
GRID = 128
NH = 768
NW = 512
N_ROW = 16
N_COL = 8


def block_scale(rng, shape, cuts, low, high):
    def one(dim, parts):
        draws = jax.random.uniform(jax.random.fold_in(jax.random.fold_in(rng, 6), dim), (parts,), jnp.float32, low / len(cuts), high / len(cuts))
        return jnp.repeat(jnp.exp(draws), shape[dim] // parts).reshape((-1,) + (1,) * (len(shape) - dim - 1))

    loudness = one(*cuts[0])
    for cut in cuts[1:]:
        loudness = loudness * one(*cut)
    return loudness


def scatter_about(own_key, dims, width, reach, split=(), held_as=jnp.bfloat16):
    result = jax.random.normal(own_key, dims, jnp.float32) * width
    if len(split) > 0:
        result = block_scale(own_key, dims, split, -0.22, 0.18) * result
    return jnp.clip(result, min=-reach, max=reach).astype(held_as)


def setup_inputs(seed: int = 0) -> dict:
    key_of = jax.random.split(jax.random.key(seed), 11)
    image = scatter_about(key_of[0], (NH, NW, C), 1.0, 6.0, ((0, 16), (1, 8)))
    norm_gain = jnp.clip(1.0 + 0.18 * jax.random.normal(key_of[1], (LAYERS, 2, C), jnp.float32), 0.1, 1.9)
    conv_first = scatter_about(key_of[2], (LAYERS, 3, 3, C, C), (9 * C) ** -0.5, 0.125)
    conv_second = scatter_about(key_of[3], (LAYERS, 3, 3, C, C), (9 * C) ** -0.5, 0.125)
    proj_in = scatter_about(key_of[4], (LAYERS, C, 2 * C), C ** -0.5, 0.375)
    block_mix = scatter_about(key_of[5], (LAYERS, POSITIONS, POSITIONS), POSITIONS ** -0.5, 0.375)
    block_bias = jnp.clip(jax.random.uniform(key_of[6], (LAYERS, POSITIONS), jnp.float32, 0.5, 1.5), 0.5, 1.5)
    grid_mix = scatter_about(key_of[7], (LAYERS, GRID, GRID), GRID ** -0.5, 0.5)
    grid_bias = jnp.clip(jax.random.uniform(key_of[8], (LAYERS, GRID), jnp.float32, 0.5, 1.5), 0.5, 1.5)
    proj_out = scatter_about(key_of[9], (LAYERS, C, C), C ** -0.5, 0.375)
    return {"image": image, "norm_gain": norm_gain, "conv_first": conv_first, "conv_second": conv_second, "proj_in": proj_in, "block_mix": block_mix, "block_bias": block_bias, "grid_mix": grid_mix, "grid_bias": grid_bias, "proj_out": proj_out}


epsilon = 1e-06

def layer_norm(field, gain_vector):
    values = field.astype(jnp.float32)
    average = lax.optimization_barrier(jnp.mean(values, axis=-1, keepdims=True))
    centred = values - average
    variance = lax.optimization_barrier(jnp.mean(centred * centred, axis=-1, keepdims=True))
    return centred * lax.rsqrt(variance + epsilon) * gain_vector

def convolve(padded, kernel, out_rows, out_cols):
    channels = padded.shape[-1]
    accumulated = jnp.zeros((out_rows * out_cols, kernel.shape[-1]), jnp.float32)
    for offset_row in range(3):
        for offset_col in range(3):
            window = padded[offset_row:offset_row + out_rows, offset_col:offset_col + out_cols].reshape(-1, channels)
            accumulated = accumulated + jnp.dot(window, kernel[offset_row, offset_col], preferred_element_type=jnp.float32)
    return accumulated.reshape(out_rows, out_cols, kernel.shape[-1])

def reference(image, norm_gain, conv_first, conv_second, proj_in, block_mix, block_bias, grid_mix, grid_bias, proj_out):
    height = CH * N_ROW
    breadth = CW * N_COL
    half_width = C // 2
    grid_cells = N_ROW * N_COL
    current = image
    for which_layer in range(LAYERS):
        normed = layer_norm(current, norm_gain[which_layer, 0]).astype(jnp.bfloat16)
        padded = jnp.pad(normed, ((1, 1), (1, 1), (0, 0)))
        first_conv = jax.nn.gelu(convolve(padded, conv_first[which_layer], height, breadth)).astype(jnp.bfloat16)
        padded_first = jnp.pad(first_conv, ((1, 1), (1, 1), (0, 0)))
        second_conv = convolve(padded_first, conv_second[which_layer], height, breadth)
        mixed_state = current.astype(jnp.float32) + second_conv
        normed_two = layer_norm(mixed_state, norm_gain[which_layer, 1]).astype(jnp.bfloat16).reshape(-1, C)
        expanded = jax.nn.gelu(jnp.dot(normed_two, proj_in[which_layer], preferred_element_type=jnp.float32)).astype(jnp.bfloat16)
        local_u = expanded[:, :half_width]
        local_v = expanded[:, half_width:C]
        global_u = expanded[:, C:C + half_width]
        global_v = expanded[:, C + half_width:]
        local_flat = local_v.reshape(height // BLOCK, BLOCK, breadth // BLOCK, BLOCK, half_width)
        local_flat = local_flat.transpose(1, 3, 0, 2, 4).reshape(BLOCK * BLOCK, -1)
        local_mixed = jnp.dot(block_mix[which_layer], local_flat, preferred_element_type=jnp.float32) + block_bias[which_layer][:, None]
        local_mixed = local_mixed.reshape(BLOCK, BLOCK, height // BLOCK, breadth // BLOCK, half_width)
        local_mixed = local_mixed.transpose(2, 0, 3, 1, 4).reshape(-1, half_width)
        gated_local = (local_u.astype(jnp.float32) * local_mixed).astype(jnp.bfloat16)
        global_flat = global_v.reshape(N_ROW, CH, N_COL, CW, half_width).transpose(0, 2, 1, 3, 4).reshape(grid_cells, -1)
        global_mixed = jnp.dot(grid_mix[which_layer], global_flat, preferred_element_type=jnp.float32) + grid_bias[which_layer][:, None]
        global_mixed = lax.optimization_barrier(global_mixed.astype(jnp.bfloat16))
        global_mixed = global_mixed.reshape(N_ROW, N_COL, CH, CW, half_width).transpose(0, 2, 1, 3, 4).reshape(-1, half_width)
        gated_global = (global_u.astype(jnp.float32) * global_mixed.astype(jnp.float32)).astype(jnp.bfloat16)
        joined = jnp.concatenate([gated_local, gated_global], axis=-1)
        projected = jnp.dot(joined, proj_out[which_layer], preferred_element_type=jnp.float32)
        current = (mixed_state + projected.reshape(height, breadth, C)).astype(jnp.bfloat16)
    return current
```

```python
import functools

import jax
import jax.numpy as jnp
from jax import lax
from jax.experimental import pallas as pl
from jax.experimental.pallas import tpu as pltpu
from jax.sharding import PartitionSpec as P

MESH = pl.DeviceIdType.MESH
F32 = jnp.float32
BF16 = jnp.bfloat16
LAYERS = 2
CH, CW, C, H = 48, 64, 256, 128
PIX = CH * CW
NROW, NCOL, CELLS = 16, 8, 128
SHARE = PIX // CELLS
OCT = SHARE // 8
EPS = 1e-06
GA = 0.7978845608028654
GB = GA * 0.044715


def gelu(v):
    h = 0.5 * v
    return h + h * jnp.tanh(v * (GA + GB * (v * v)))


def norm(v, gain):
    mean = jnp.sum(v, axis=-1, keepdims=True) * (1.0 / C)
    centred = v - mean
    var = jnp.sum(centred * centred, axis=-1, keepdims=True) * (1.0 / C)
    return centred * lax.rsqrt(var + EPS) * gain


def put_row(dst, u, y, left, right):
    at = pl.ds(pl.multiple_of(u * CW, CW), CW)
    j = lax.broadcasted_iota(jnp.int32, (CW, C), 0)
    dst[at, 0:C] = jnp.where(j == 0, left, pltpu.roll(y, 1, 0)).astype(BF16)
    dst[at, C : 2 * C] = y.astype(BF16)
    dst[at, 2 * C : 3 * C] = jnp.where(j == CW - 1, right, pltpu.roll(y, CW - 1, 0)).astype(BF16)


def kernel(
    image, gains, k1_hbm, k2_hbm, pin_hbm, bm_hbm, gm_hbm, pout_hbm, bbias, gbias,
    cur,
    k1, k2, pin, bmix, gmix, pout,
    X, F, MS, LU, LV, GU, GV, J, CBF, CB, HC, HV, HLF, RF, RECV, S32, MIX, GMV,
    w_sem, im_sem, hs_sem, hr_sem, as_sem, ar_sem, bs_sem, br_sem,
):
    row, col = lax.axis_index("row"), lax.axis_index("col")
    core = row % 2
    me = row * NCOL + col
    chip = (row // 2) * NCOL + col
    share = core * 64 + chip
    y0, xh, xl, z0 = row // 4, (row // 2) % 2, col // 4, col % 4

    def peer(k):
        k = (k * 37) % 64
        y = (y0 + k // 16) % 4
        h = (xh + (k // 8) % 2) % 2
        w = (xl + (k // 4) % 2) % 2
        z = (z0 + k % 4) % 4
        return y * 2 + h, w * 4 + z

    weights = ((k1_hbm, k1), (k2_hbm, k2), (pin_hbm, pin), (bm_hbm, bmix), (gm_hbm, gmix), (pout_hbm, pout))

    def weight(i, l):
        src, dst = weights[i]
        return pltpu.make_async_copy(src.at[l], dst.at[l], w_sem.at[l, i])

    load_image = pltpu.make_async_copy(image, cur, im_sem.at[0])
    load_image.start()
    for l in range(LAYERS):
        for i in range(len(weights)):
            weight(i, l).start()

    barrier = pltpu.get_barrier_semaphore()

    for kappa in range(2):

        def greet(k, carry):
            r2, c2 = peer(k)
            pl.semaphore_signal(barrier, inc=1, device_id=(r2 * 2 + kappa, c2), device_id_type=MESH)
            return carry

        lax.fori_loop((core == kappa).astype(jnp.int32), 64, greet, 0)

    load_image.wait()
    zero_row = jnp.zeros((1, C), F32)

    def layer(l, carry):
        gain0 = gains[pl.ds(2 * l, 1), :]
        gain1 = gains[pl.ds(2 * l + 1, 1), :]

        def norm_rows(c, carry):
            v = cur[pl.ds(pl.multiple_of(c * 256, 256), 256), :].astype(F32)
            n = norm(v, gain0)
            for r in range(4):
                y = n[r * CW : (r + 1) * CW]
                i = c * 4 + r
                put_row(X, i + 2, y, zero_row, zero_row)
                for slot, j in enumerate((0, 1, CW - 2, CW - 1)):
                    CBF[slot, pl.ds(i + 16, 1), :] = y[j : j + 1]
            return carry

        lax.fori_loop(0, CH // 4, norm_rows, 0)
        CB[...] = CBF[:, 16:64, :].astype(BF16)

        @pl.when(l == 0)
        def _():
            pl.semaphore_wait(barrier, CELLS - 1)

        up, down = (row + NROW - 1) % NROW, (row + 1) % NROW
        left, right = (col + NCOL - 1) % NCOL, (col + 1) % NCOL
        plan = (
            (X.at[2 * CW : 4 * CW, C : 2 * C], HV.at[l, 1], up, col),
            (X.at[CH * CW : (CH + 2) * CW, C : 2 * C], HV.at[l, 0], down, col),
            (CB.at[0:2], HC.at[l, 1, :, 16:64], row, left),
            (CB.at[2:4], HC.at[l, 0, :, 16:64], row, right),
            (CB.at[0:2, 0:16], HC.at[l, 1, :, 64:80], up, left),
            (CB.at[2:4, 0:16], HC.at[l, 0, :, 64:80], up, right),
            (CB.at[0:2, 32:48], HC.at[l, 1, :, 0:16], down, left),
            (CB.at[2:4, 32:48], HC.at[l, 0, :, 0:16], down, right),
        )
        halo = [
            pltpu.make_async_remote_copy(
                src_ref=src, dst_ref=dst, send_sem=hs_sem.at[l, i], recv_sem=hr_sem.at[l, i],
                device_id=(r, c), device_id_type=MESH,
            )
            for i, (src, dst, r, c) in enumerate(plan)
        ]
        for copy in halo:
            copy.start()
        weight(0, l).wait()
        for copy in halo:
            copy.wait()

        t80 = lax.broadcasted_iota(jnp.int32, (80, C), 0)
        outside = ((t80 < 16) & (row == 0)) | ((t80 >= 64) & (row == NROW - 1))
        for side, edge in ((0, col == 0), (1, col == NCOL - 1)):
            for k in range(2):
                HLF[side, k] = jnp.where(outside | edge, 0.0, HC[l, side, k].astype(F32))
        for u, part, edge in ((0, 0, row == 0), (1, 0, row == 0), (50, 1, row == NROW - 1), (51, 1, row == NROW - 1)):
            p = u % 2
            y = jnp.where(edge, 0.0, HV[l, part, p * CW : (p + 1) * CW, :].astype(F32))
            b = u + 14
            CBF[0, b : b + 1, :] = y[0:1]
            CBF[3, b : b + 1, :] = y[CW - 1 : CW]
            put_row(X, u, y, HLF[0, 1, b : b + 1, :], HLF[1, 0, b : b + 1, :])

        s16 = lax.broadcasted_iota(jnp.int32, (16, C), 0)

        def patch(i, carry):
            base = pl.multiple_of((i + 2) * CW, CW)
            a = X[pl.ds(base, 16), 0:C].astype(F32)
            X[pl.ds(base, 16), 0:C] = jnp.where(s16 == 0, HLF[0, 1, pl.ds(i + 16, 1), :], a).astype(BF16)
            b = X[pl.ds(base + CW - 16, 16), 2 * C :].astype(F32)
            X[pl.ds(base + CW - 16, 16), 2 * C :] = jnp.where(
                s16 == 15, HLF[1, 0, pl.ds(i + 16, 1), :], b
            ).astype(BF16)
            return carry

        lax.fori_loop(0, CH, patch, 0, unroll=4)

        acc = jnp.zeros((128, C), F32)
        for a in range(3):
            rows = slice(14 + a, 78 + a)
            lhs_left = jnp.concatenate([HLF[0, 0, rows, :], HLF[0, 1, rows, :], CBF[0, rows, :]], axis=1)
            lhs_right = jnp.concatenate([CBF[3, rows, :], HLF[1, 0, rows, :], HLF[1, 1, rows, :]], axis=1)
            lhs = jnp.concatenate([lhs_left, lhs_right], axis=0).astype(BF16)
            acc = acc + jnp.dot(lhs, k1[l, a * 768 : (a + 1) * 768, :], preferred_element_type=F32)
        rim = gelu(acc)
        t64 = lax.broadcasted_iota(jnp.int32, (64, C), 0)
        off = ((t64 == 0) & (row == 0)) | ((t64 == 49) & (row == NROW - 1))
        RF[0] = jnp.where(off | (col == 0), 0.0, rim[0:64])
        RF[1] = jnp.where(off | (col == NCOL - 1), 0.0, rim[64:128])

        def conv1(c, carry):
            base = c * 5
            lhs = jnp.concatenate(
                [X[pl.ds(pl.multiple_of((base + a) * CW, CW), 5 * CW), :] for a in range(3)], axis=1
            )
            y = gelu(jnp.dot(lhs, k1[l], preferred_element_type=F32))
            for r in range(5):
                t = base + r
                gone = ((t == 0) & (row == 0)) | ((t == CH + 1) & (row == NROW - 1))
                yr = jnp.where(gone, 0.0, y[r * CW : (r + 1) * CW])
                put_row(F, t, yr, RF[0, pl.ds(t, 1), :], RF[1, pl.ds(t, 1), :])
            return carry

        lax.fori_loop(0, 10, conv1, 0)
        weight(1, l).wait()
        weight(2, l).wait()

        def conv2(c, carry):
            at = pl.ds(pl.multiple_of(c * 256, 256), 256)
            lhs = jnp.concatenate(
                [F[pl.ds(pl.multiple_of((c * 4 + a) * CW, CW), 4 * CW), :] for a in range(3)], axis=1
            )
            m = cur[at, :].astype(F32) + jnp.dot(lhs, k2[l], preferred_element_type=F32)
            MS[at, :] = m
            n = norm(m, gain1).astype(BF16)
            e = gelu(jnp.dot(n, pin[l], preferred_element_type=F32))
            LU[at, :] = e[:, 0:H].astype(BF16)
            LV[at, :] = e[:, H : 2 * H].astype(BF16)
            GU[at, :] = e[:, 2 * H : 3 * H].astype(BF16)
            GV[l, pl.ds(pl.multiple_of(c * 32, 32), 32)] = e[:, 3 * H :].reshape(32, 8, H).astype(BF16)
            return carry

        def shares(c, kappa):
            return pl.ds(c * OCT, OCT)

        for kappa in range(2):
            lax.fori_loop(6 * kappa, 6 * kappa + 6, conv2, 0)

            def send(k, carry):
                r2, c2 = peer(k)
                d = kappa * 64 + r2 * NCOL + c2
                pltpu.make_async_remote_copy(
                    src_ref=GV.at[l, pl.ds(d * OCT, OCT)], dst_ref=RECV.at[l, pl.ds(me * OCT, OCT)],
                    send_sem=as_sem.at[l], recv_sem=ar_sem.at[l],
                    device_id=(r2 * 2 + kappa, c2), device_id_type=MESH,
                ).start()
                return carry

            lax.fori_loop((core == kappa).astype(jnp.int32), 64, send, 0)

        def mix():
            RECV[l, pl.ds(me * OCT, OCT)] = GV[l, pl.ds(share * OCT, OCT)]
            whole = RECV.at[l, pl.ds(0, (CELLS - 1) * OCT)]
            pltpu.make_async_copy(whole, whole, ar_sem.at[l]).wait()
            S32[...] = RECV[l].astype(F32).reshape(PIX, H)
            bias = jnp.broadcast_to(gbias[pl.ds(l, 1), :], (CELLS, CELLS)).T
            for q in range(0, SHARE, 4):
                rhs = jnp.concatenate(
                    [S32[pl.ds(q + i, CELLS, stride=SHARE), :].astype(BF16) for i in range(4)], axis=1
                )
                out = jnp.dot(gmix[l], rhs, preferred_element_type=F32)
                for i in range(4):
                    S32[pl.ds(q + i, CELLS, stride=SHARE), :] = out[:, i * H : (i + 1) * H] + bias
            MIX[l] = S32[...].reshape(CELLS * OCT, 8, H).astype(BF16)
            GMV[l, pl.ds(share * OCT, OCT)] = MIX[l, pl.ds(me * OCT, OCT)]
            for kappa in range(2):

                def back(k, carry):
                    r2, c2 = peer(k)
                    g = (r2 * 2 + kappa) * NCOL + c2
                    pltpu.make_async_remote_copy(
                        src_ref=MIX.at[l, pl.ds(g * OCT, OCT)], dst_ref=GMV.at[l, pl.ds(share * OCT, OCT)],
                        send_sem=bs_sem.at[l], recv_sem=br_sem.at[l, core],
                        device_id=(r2 * 2 + kappa, c2), device_id_type=MESH,
                    ).start()
                    return carry

                lax.fori_loop((core == kappa).astype(jnp.int32), 64, back, 0)

        weight(3, l).wait()
        weight(4, l).wait()
        weight(5, l).wait()
        pl.when(core == 0)(mix)

        lbias = jnp.broadcast_to(bbias[pl.ds(l, 1), :], (H, C)).T

        def block(s, carry):
            for half in range(2):
                cols = [slice((2 * half + i) * 16, (2 * half + i + 1) * 16) for i in range(2)]

                def rows(r, cs):
                    return pl.ds(pl.multiple_of((s * 16 + r) * CW + cs.start, 16), 16)

                rhs = jnp.concatenate(
                    [jnp.concatenate([LV[rows(r, cs), :] for r in range(16)], axis=0) for cs in cols], axis=1
                )
                lm = jnp.dot(bmix[l], rhs, preferred_element_type=F32)
                for i, cs in enumerate(cols):
                    for r in range(16):
                        part = lm[r * 16 : (r + 1) * 16, i * H : (i + 1) * H] + lbias[r * 16 : (r + 1) * 16]
                        J[rows(r, cs), 0:H] = (LU[rows(r, cs), :].astype(F32) * part).astype(BF16)
            return carry

        lax.fori_loop(0, CH // 16, block, 0)
        pl.when(core == 1)(mix)

        def finish(c, carry):
            at = pl.ds(pl.multiple_of(c * 256, 256), 256)
            gm = GMV[l, pl.ds(pl.multiple_of(c * 32, 32), 32)].astype(F32).reshape(256, H)
            gated = (GU[at, :].astype(F32) * gm).astype(BF16)
            joined = jnp.concatenate([J[at, 0:H], gated], axis=1)
            out = jnp.dot(joined, pout[l], preferred_element_type=F32)
            cur[at, :] = (MS[at, :] + out).astype(BF16)
            return carry

        for kappa in range(2):
            for own in range(2):

                @pl.when(core == own)
                def _():
                    some = GMV.at[l, pl.ds(0, (64 - (own == kappa)) * OCT)]
                    pltpu.make_async_copy(some, some, br_sem.at[l, kappa]).wait()

            lax.fori_loop(6 * kappa, 6 * kappa + 6, finish, 0)

        whole = GV.at[l, pl.ds(0, (CELLS - 1) * OCT)]
        pltpu.make_async_copy(whole, whole, as_sem.at[l]).wait()
        whole = MIX.at[l, pl.ds(0, (CELLS - 1) * OCT)]
        pltpu.make_async_copy(whole, whole, bs_sem.at[l]).wait()
        return carry

    lax.fori_loop(0, LAYERS, layer, 0)


def on_device(image, norm_gain, conv_first, conv_second, proj_in, block_mix, block_bias, grid_mix, grid_bias, proj_out):
    any_space = pl.BlockSpec(memory_space=pl.ANY)
    vmem = pl.BlockSpec(memory_space=pltpu.VMEM)
    V = pltpu.VMEM
    DMA = pltpu.SemaphoreType.DMA
    scratch = [
        V((LAYERS, 9 * C, C), BF16), V((LAYERS, 9 * C, C), BF16), V((LAYERS, C, 2 * C), BF16),
        V((LAYERS, C, C), BF16), V((LAYERS, CELLS, CELLS), BF16), V((LAYERS, C, C), BF16),
        V(((CH + 4) * CW, 3 * C), BF16), V(((CH + 2) * CW, 3 * C), BF16), V((PIX, C), F32),
        V((PIX, H), BF16), V((PIX, H), BF16), V((PIX, H), BF16), V((LAYERS, PIX // 8, 8, H), BF16), V((PIX, H), BF16),
        V((4, 80, C), F32), V((4, CH, C), BF16), V((LAYERS, 2, 2, 80, C), BF16), V((LAYERS, 2, 2 * CW, C), BF16),
        V((2, 2, 80, C), F32), V((2, 64, C), F32),
        V((LAYERS, PIX // 8, 8, H), BF16), V((PIX, H), F32), V((LAYERS, PIX // 8, 8, H), BF16),
        V((LAYERS, PIX // 8, 8, H), BF16),
        DMA((LAYERS, 6)), DMA((1,)), DMA((LAYERS, 8)), DMA((LAYERS, 8)),
        DMA((LAYERS,)), DMA((LAYERS,)), DMA((LAYERS,)), DMA((LAYERS, 2)),
    ]
    out = pl.pallas_call(
        kernel,
        out_shape=jax.ShapeDtypeStruct((PIX, C), BF16),
        in_specs=[any_space, vmem] + [any_space] * 6 + [vmem, vmem],
        out_specs=vmem,
        scratch_shapes=scratch,
        compiler_params=pltpu.CompilerParams(
            collective_id=0, has_side_effects=True, vmem_limit_bytes=62 * 2**20
        ),
    )(
        image.reshape(PIX, C), norm_gain.reshape(2 * LAYERS, C),
        conv_first.reshape(LAYERS, 9 * C, C), conv_second.reshape(LAYERS, 9 * C, C),
        proj_in, block_mix, grid_mix, proj_out, block_bias, grid_bias,
    )
    return out.reshape(image.shape)


def solution(mesh):
    placed = (P("row", "col", None), P(), P(), P(), P(), P(), P(), P(), P(), P())
    return jax.shard_map(
        on_device, mesh=mesh, in_specs=placed, out_specs=P("row", "col", None), check_vma=False
    )
```

```python
import functools

import jax
import jax.numpy as jnp
from jax import lax
from jax.experimental import pallas as pl
from jax.experimental.pallas import tpu as pltpu
from jax.sharding import PartitionSpec as P

MESH = pl.DeviceIdType.MESH
F32 = jnp.float32
BF16 = jnp.bfloat16
LAYERS = 2
CH, CW, C, H = 48, 64, 256, 128
PIX = CH * CW
NROW, NCOL, CELLS = 16, 8, 128
SHARE = PIX // CELLS
OCT = SHARE // 8
EPS = 1e-06
GA = 0.7978845608028654
GB = GA * 0.044715


def gelu(v):
    h = 0.5 * v
    return h + h * jnp.tanh(v * (GA + GB * (v * v)))


def norm(v, gain):
    mean = jnp.sum(v, axis=-1, keepdims=True) * (1.0 / C)
    centred = v - mean
    var = jnp.sum(centred * centred, axis=-1, keepdims=True) * (1.0 / C)
    return centred * lax.rsqrt(var + EPS) * gain


def put_row(dst, u, y, left, right):
    at = pl.ds(pl.multiple_of(u * CW, CW), CW)
    j = lax.broadcasted_iota(jnp.int32, (CW, C), 0)
    dst[at, 0:C] = jnp.where(j == 0, left, pltpu.roll(y, 1, 0)).astype(BF16)
    dst[at, C : 2 * C] = y.astype(BF16)
    dst[at, 2 * C : 3 * C] = jnp.where(j == CW - 1, right, pltpu.roll(y, CW - 1, 0)).astype(BF16)


def kernel(
    image, gains, k1_hbm, k2_hbm, pin_hbm, bm_hbm, gm_hbm, pout_hbm, bbias, gbias,
    cur,
    k1, k2, pin, bmix, gmix, pout,
    X, F, MS, LU, LV, GU, GV, J, CBF, CB, HC, HV, HLF, RF, RECV, S32, MIX, GMV, A0, A1, B0, B1, E0, E1,
    w_sem, im_sem, hs_sem, hr_sem, as_sem, ar_sem, bs_sem, br_sem,
):
    row, col = lax.axis_index("row"), lax.axis_index("col")
    core = row % 2
    me = row * NCOL + col
    chip = (row // 2) * NCOL + col
    share = core * 64 + chip
    y0, xh, xl, z0 = row // 4, (row // 2) % 2, col // 4, col % 4

    def peer(k):
        k = (k * 37) % 64
        y = (y0 + k // 16) % 4
        h = (xh + (k // 8) % 2) % 2
        w = (xl + (k // 4) % 2) % 2
        z = (z0 + k % 4) % 4
        return y * 2 + h, w * 4 + z

    def to_group(kappa, act):
        @pl.when(core != kappa)
        def _():
            act(0)

        def step(k, carry):
            act(k)
            return carry

        lax.fori_loop(1, 64, step, 0, unroll=7)

    weights = ((k1_hbm, k1), (k2_hbm, k2), (pin_hbm, pin), (bm_hbm, bmix), (gm_hbm, gmix), (pout_hbm, pout))

    def weight(i, l):
        src, dst = weights[i]
        return pltpu.make_async_copy(src.at[l], dst.at[l], w_sem.at[l, i])

    load_image = pltpu.make_async_copy(image, cur, im_sem.at[0])
    load_image.start()
    for l in range(LAYERS):
        for i in range(len(weights)):
            weight(i, l).start()

    barrier = pltpu.get_barrier_semaphore()

    for kappa in range(2):

        def greet(k):
            r2, c2 = peer(k)
            pl.semaphore_signal(barrier, inc=1, device_id=(r2 * 2 + kappa, c2), device_id_type=MESH)

        to_group(kappa, greet)

    load_image.wait()
    zero_row = jnp.zeros((1, C), F32)

    def layer(l, carry):
        gain0 = gains[l, 0:1, :]
        gain1 = gains[l, 1:2, :]

        def norm_rows(c, carry):
            v = cur[pl.ds(pl.multiple_of(c * 256, 256), 256), :].astype(F32)
            n = norm(v, gain0)
            for r in range(4):
                y = n[r * CW : (r + 1) * CW]
                i = c * 4 + r
                put_row(X, i + 2, y, zero_row, zero_row)
                for slot, j in enumerate((0, 1, CW - 2, CW - 1)):
                    CBF[slot, pl.ds(i + 16, 1), :] = y[j : j + 1]
            return carry

        lax.fori_loop(0, CH // 4, norm_rows, 0, unroll=2)
        CB[...] = CBF[:, 16:64, :].astype(BF16)

        @pl.when(l == 0)
        def _():
            pl.semaphore_wait(barrier, CELLS - 1)

        up, down = (row + NROW - 1) % NROW, (row + 1) % NROW
        left, right = (col + NCOL - 1) % NCOL, (col + 1) % NCOL
        plan = (
            (X.at[2 * CW : 4 * CW, C : 2 * C], HV.at[l, 1], up, col),
            (X.at[CH * CW : (CH + 2) * CW, C : 2 * C], HV.at[l, 0], down, col),
            (CB.at[0:2], HC.at[l, 1, :, 16:64], row, left),
            (CB.at[2:4], HC.at[l, 0, :, 16:64], row, right),
            (CB.at[0:2, 0:16], HC.at[l, 1, :, 64:80], up, left),
            (CB.at[2:4, 0:16], HC.at[l, 0, :, 64:80], up, right),
            (CB.at[0:2, 32:48], HC.at[l, 1, :, 0:16], down, left),
            (CB.at[2:4, 32:48], HC.at[l, 0, :, 0:16], down, right),
        )
        halo = [
            pltpu.make_async_remote_copy(
                src_ref=src, dst_ref=dst, send_sem=hs_sem.at[l, i], recv_sem=hr_sem.at[l, i],
                device_id=(r, c), device_id_type=MESH,
            )
            for i, (src, dst, r, c) in enumerate(plan)
        ]
        for copy in halo:
            copy.start()
        weight(0, l).wait()
        for copy in halo:
            copy.wait()

        t80 = lax.broadcasted_iota(jnp.int32, (80, C), 0)
        outside = ((t80 < 16) & (row == 0)) | ((t80 >= 64) & (row == NROW - 1))
        for side, edge in ((0, col == 0), (1, col == NCOL - 1)):
            for k in range(2):
                HLF[side, k] = jnp.where(outside | edge, 0.0, HC[l, side, k].astype(F32))
        for u, part, edge in ((0, 0, row == 0), (1, 0, row == 0), (50, 1, row == NROW - 1), (51, 1, row == NROW - 1)):
            p = u % 2
            y = jnp.where(edge, 0.0, HV[l, part, p * CW : (p + 1) * CW, :].astype(F32))
            b = u + 14
            CBF[0, b : b + 1, :] = y[0:1]
            CBF[3, b : b + 1, :] = y[CW - 1 : CW]
            put_row(X, u, y, HLF[0, 1, b : b + 1, :], HLF[1, 0, b : b + 1, :])

        s16 = lax.broadcasted_iota(jnp.int32, (16, C), 0)

        def patch(i, carry):
            base = pl.multiple_of((i + 2) * CW, CW)
            a = X[pl.ds(base, 16), 0:C].astype(F32)
            X[pl.ds(base, 16), 0:C] = jnp.where(s16 == 0, HLF[0, 1, pl.ds(i + 16, 1), :], a).astype(BF16)
            b = X[pl.ds(base + CW - 16, 16), 2 * C :].astype(F32)
            X[pl.ds(base + CW - 16, 16), 2 * C :] = jnp.where(
                s16 == 15, HLF[1, 0, pl.ds(i + 16, 1), :], b
            ).astype(BF16)
            return carry

        lax.fori_loop(0, CH, patch, 0, unroll=4)

        acc = jnp.zeros((128, C), F32)
        for a in range(3):
            rows = slice(14 + a, 78 + a)
            lhs_left = jnp.concatenate([HLF[0, 0, rows, :], HLF[0, 1, rows, :], CBF[0, rows, :]], axis=1)
            lhs_right = jnp.concatenate([CBF[3, rows, :], HLF[1, 0, rows, :], HLF[1, 1, rows, :]], axis=1)
            lhs = jnp.concatenate([lhs_left, lhs_right], axis=0).astype(BF16)
            acc = acc + jnp.dot(lhs, k1[l, a * 768 : (a + 1) * 768, :], preferred_element_type=F32)
        rim = gelu(acc)
        t64 = lax.broadcasted_iota(jnp.int32, (64, C), 0)
        off = ((t64 == 0) & (row == 0)) | ((t64 == 49) & (row == NROW - 1))
        RF[0] = jnp.where(off | (col == 0), 0.0, rim[0:64])
        RF[1] = jnp.where(off | (col == NCOL - 1), 0.0, rim[64:128])

        def conv1_dot(c, acc):
            base = c * 5
            lhs = jnp.concatenate(
                [X[pl.ds(pl.multiple_of((base + a) * CW, CW), 5 * CW), :] for a in range(3)], axis=1
            )
            acc[...] = jnp.dot(lhs, k1[l], preferred_element_type=F32)

        def conv1_rows(c, acc):
            for r in range(5):
                t = c * 5 + r
                gone = ((t == 0) & (row == 0)) | ((t == CH + 1) & (row == NROW - 1))
                y = jnp.where(gone, 0.0, gelu(acc[r * CW : (r + 1) * CW, :]))
                put_row(F, t, y, RF[0, pl.ds(t, 1), :], RF[1, pl.ds(t, 1), :])

        def conv1_pair(p, carry):
            conv1_dot(2 * p + 1, A1)
            conv1_rows(2 * p, A0)
            conv1_dot(jnp.minimum(2 * p + 2, 9), A0)
            conv1_rows(2 * p + 1, A1)
            return carry

        def conv2_dot(c, acc):
            lhs = jnp.concatenate(
                [F[pl.ds(pl.multiple_of((c * 4 + a) * CW, CW), 4 * CW), :] for a in range(3)], axis=1
            )
            acc[...] = jnp.dot(lhs, k2[l], preferred_element_type=F32)

        def conv2_norm(c, acc, e):
            at = pl.ds(pl.multiple_of(c * 256, 256), 256)
            m = cur[at, :].astype(F32) + acc[...]
            MS[at, :] = m
            n = norm(m, gain1).astype(BF16)
            e[...] = jnp.dot(n, pin[l], preferred_element_type=F32)

        def conv2_gelu(c, e):
            at = pl.ds(pl.multiple_of(c * 256, 256), 256)
            for h, dst in enumerate((LU, LV, GU)):
                dst[at, :] = gelu(e[:, h * H : (h + 1) * H]).astype(BF16)
            GV[l, pl.ds(pl.multiple_of(c * 32, 32), 32)] = gelu(e[:, 3 * H :]).reshape(32, 8, H).astype(BF16)

        weight(1, l).wait()
        weight(2, l).wait()
        conv1_dot(0, A0)

        for kappa in range(2):
            lax.fori_loop(3 * kappa, 3 + 2 * kappa, conv1_pair, 0)
            accs, es = (B0, B1), (E0, E1)
            first = 6 * kappa
            for i in range(8):
                if i < 6:
                    conv2_dot(first + i, accs[i % 2])
                if 1 <= i < 7:
                    conv2_norm(first + i - 1, accs[(i - 1) % 2], es[(i - 1) % 2])
                if i >= 2:
                    conv2_gelu(first + i - 2, es[i % 2])

            def send(k):
                r2, c2 = peer(k)
                d = kappa * 64 + r2 * NCOL + c2
                pltpu.make_async_remote_copy(
                    src_ref=GV.at[l, pl.ds(d * OCT, OCT)], dst_ref=RECV.at[l, pl.ds(me * OCT, OCT)],
                    send_sem=as_sem.at[l], recv_sem=ar_sem.at[l],
                    device_id=(r2 * 2 + kappa, c2), device_id_type=MESH,
                ).start()

            to_group(kappa, send)

        def mix():
            RECV[l, pl.ds(me * OCT, OCT)] = GV[l, pl.ds(share * OCT, OCT)]
            whole = RECV.at[l, pl.ds(0, (CELLS - 1) * OCT)]
            pltpu.make_async_copy(whole, whole, ar_sem.at[l]).wait()
            S32[...] = RECV[l].astype(F32).reshape(PIX, H)
            bias = jnp.broadcast_to(gbias[pl.ds(l, 1), :], (CELLS, CELLS)).T
            for q in range(0, SHARE, 4):
                rhs = jnp.concatenate(
                    [S32[pl.ds(q + i, CELLS, stride=SHARE), :].astype(BF16) for i in range(4)], axis=1
                )
                out = jnp.dot(gmix[l], rhs, preferred_element_type=F32)
                for i in range(4):
                    S32[pl.ds(q + i, CELLS, stride=SHARE), :] = out[:, i * H : (i + 1) * H] + bias
            MIX[l] = S32[...].reshape(CELLS * OCT, 8, H).astype(BF16)
            GMV[l, pl.ds(share * OCT, OCT)] = MIX[l, pl.ds(me * OCT, OCT)]
            for kappa in range(2):

                def back(k):
                    r2, c2 = peer(k)
                    g = (r2 * 2 + kappa) * NCOL + c2
                    pltpu.make_async_remote_copy(
                        src_ref=MIX.at[l, pl.ds(g * OCT, OCT)], dst_ref=GMV.at[l, pl.ds(share * OCT, OCT)],
                        send_sem=bs_sem.at[l], recv_sem=br_sem.at[l, core],
                        device_id=(r2 * 2 + kappa, c2), device_id_type=MESH,
                    ).start()

                to_group(kappa, back)

        weight(3, l).wait()
        weight(4, l).wait()
        weight(5, l).wait()
        pl.when(core == 0)(mix)

        lbias = jnp.broadcast_to(bbias[pl.ds(l, 1), :], (H, C)).T

        def block(s, carry):
            for half in range(2):
                cols = [slice((2 * half + i) * 16, (2 * half + i + 1) * 16) for i in range(2)]

                def rows(r, cs):
                    return pl.ds(pl.multiple_of((s * 16 + r) * CW + cs.start, 16), 16)

                rhs = jnp.concatenate(
                    [jnp.concatenate([LV[rows(r, cs), :] for r in range(16)], axis=0) for cs in cols], axis=1
                )
                lm = jnp.dot(bmix[l], rhs, preferred_element_type=F32)
                for i, cs in enumerate(cols):
                    for r in range(16):
                        part = lm[r * 16 : (r + 1) * 16, i * H : (i + 1) * H] + lbias[r * 16 : (r + 1) * 16]
                        J[rows(r, cs), 0:H] = (LU[rows(r, cs), :].astype(F32) * part).astype(BF16)
            return carry

        lax.fori_loop(0, CH // 16, block, 0)
        pl.when(core == 1)(mix)

        def finish(c, carry):
            at = pl.ds(pl.multiple_of(c * 256, 256), 256)
            gm = GMV[l, pl.ds(pl.multiple_of(c * 32, 32), 32)].astype(F32).reshape(256, H)
            gated = (GU[at, :].astype(F32) * gm).astype(BF16)
            joined = jnp.concatenate([J[at, 0:H], gated], axis=1)
            out = jnp.dot(joined, pout[l], preferred_element_type=F32)
            cur[at, :] = (MS[at, :] + out).astype(BF16)
            return carry

        for kappa in range(2):
            for own in range(2):

                @pl.when(core == own)
                def _():
                    some = GMV.at[l, pl.ds(0, (64 - (own == kappa)) * OCT)]
                    pltpu.make_async_copy(some, some, br_sem.at[l, kappa]).wait()

            lax.fori_loop(6 * kappa, 6 * kappa + 6, finish, 0, unroll=2)

        whole = GV.at[l, pl.ds(0, (CELLS - 1) * OCT)]
        pltpu.make_async_copy(whole, whole, as_sem.at[l]).wait()
        whole = MIX.at[l, pl.ds(0, (CELLS - 1) * OCT)]
        pltpu.make_async_copy(whole, whole, bs_sem.at[l]).wait()
        return carry

    lax.fori_loop(0, LAYERS, layer, 0)


def on_device(image, norm_gain, conv_first, conv_second, proj_in, block_mix, block_bias, grid_mix, grid_bias, proj_out):
    any_space = pl.BlockSpec(memory_space=pl.ANY)
    vmem = pl.BlockSpec(memory_space=pltpu.VMEM)
    V = pltpu.VMEM
    DMA = pltpu.SemaphoreType.DMA
    scratch = [
        V((LAYERS, 9 * C, C), BF16), V((LAYERS, 9 * C, C), BF16), V((LAYERS, C, 2 * C), BF16),
        V((LAYERS, C, C), BF16), V((LAYERS, CELLS, CELLS), BF16), V((LAYERS, C, C), BF16),
        V(((CH + 4) * CW, 3 * C), BF16), V(((CH + 2) * CW, 3 * C), BF16), V((PIX, C), F32),
        V((PIX, H), BF16), V((PIX, H), BF16), V((PIX, H), BF16), V((LAYERS, PIX // 8, 8, H), BF16), V((PIX, H), BF16),
        V((4, 80, C), F32), V((4, CH, C), BF16), V((LAYERS, 2, 2, 80, C), BF16), V((LAYERS, 2, 2 * CW, C), BF16),
        V((2, 2, 80, C), F32), V((2, 64, C), F32),
        V((LAYERS, PIX // 8, 8, H), BF16), V((PIX, H), F32), V((LAYERS, PIX // 8, 8, H), BF16),
        V((LAYERS, PIX // 8, 8, H), BF16),
        V((5 * CW, C), F32), V((5 * CW, C), F32), V((4 * CW, C), F32), V((4 * CW, C), F32),
        V((4 * CW, 2 * C), F32), V((4 * CW, 2 * C), F32),
        DMA((LAYERS, 6)), DMA((1,)), DMA((LAYERS, 8)), DMA((LAYERS, 8)),
        DMA((LAYERS,)), DMA((LAYERS,)), DMA((LAYERS,)), DMA((LAYERS, 2)),
    ]
    out = pl.pallas_call(
        kernel,
        out_shape=jax.ShapeDtypeStruct((PIX, C), BF16),
        in_specs=[any_space, vmem] + [any_space] * 6 + [vmem, vmem],
        out_specs=vmem,
        scratch_shapes=scratch,
        compiler_params=pltpu.CompilerParams(
            collective_id=0, has_side_effects=True, vmem_limit_bytes=62 * 2**20
        ),
    )(
        image.reshape(PIX, C), norm_gain,
        conv_first.reshape(LAYERS, 9 * C, C), conv_second.reshape(LAYERS, 9 * C, C),
        proj_in, block_mix, grid_mix, proj_out, block_bias, grid_bias,
    )
    return out.reshape(image.shape)


def solution(mesh):
    placed = (P("row", "col", None), P(), P(), P(), P(), P(), P(), P(), P(), P())
    return jax.shard_map(
        on_device, mesh=mesh, in_specs=placed, out_specs=P("row", "col", None), check_vma=False
    )
```

```python
import functools

import jax
import jax.numpy as jnp
from jax import lax
from jax.experimental import pallas as pl
from jax.experimental.pallas import tpu as pltpu
from jax.sharding import PartitionSpec as P

MESH = pl.DeviceIdType.MESH
F32 = jnp.float32
BF16 = jnp.bfloat16
LAYERS = 2
CH, CW, C, H = 48, 64, 256, 128
PIX = CH * CW
NROW, NCOL, CELLS = 16, 8, 128
SHARE = PIX // CELLS
OCT = SHARE // 8
EPS = 1e-06
GA = 0.7978845608028654
GB = GA * 0.044715


def gelu(v):
    h = 0.5 * v
    return h + h * jnp.tanh(v * (GA + GB * (v * v)))


def norm(v, gain):
    mean = jnp.sum(v, axis=-1, keepdims=True) * (1.0 / C)
    centred = v - mean
    var = jnp.sum(centred * centred, axis=-1, keepdims=True) * (1.0 / C)
    return centred * lax.rsqrt(var + EPS) * gain


def put_row(dst, u, y, left, right):
    at = pl.ds(pl.multiple_of(u * CW, CW), CW)
    j = lax.broadcasted_iota(jnp.int32, (CW, C), 0)
    dst[at, 0:C] = jnp.where(j == 0, left, pltpu.roll(y, 1, 0)).astype(BF16)
    dst[at, C : 2 * C] = y.astype(BF16)
    dst[at, 2 * C : 3 * C] = jnp.where(j == CW - 1, right, pltpu.roll(y, CW - 1, 0)).astype(BF16)


def kernel(
    image, gains, k1_hbm, k2_hbm, pin_hbm, bm_hbm, gm_hbm, pout_hbm, bbias, gbias,
    cur,
    k1, k2, pin, bmix, gmix, pout,
    X, F, MS, LU, LV, GU, GV, J, CBF, CB, HC, HV, HLF, RF, RECV, S32, MIX, GMV, A0, A1, B0, B1, E0, E1,
    w_sem, im_sem, hs_sem, hr_sem, as_sem, ar_sem, bs_sem, br_sem,
):
    row, col = lax.axis_index("row"), lax.axis_index("col")
    core = row % 2
    me = row * NCOL + col
    chip = (row // 2) * NCOL + col
    share = core * 64 + chip
    y0, xh, xl, z0 = row // 4, (row // 2) % 2, col // 4, col % 4

    def peer(k):
        k = (k * 37) % 64
        y = (y0 + k // 16) % 4
        h = (xh + (k // 8) % 2) % 2
        w = (xl + (k // 4) % 2) % 2
        z = (z0 + k % 4) % 4
        return y * 2 + h, w * 4 + z

    def to_group(kappa, act):
        @pl.when(core != kappa)
        def _():
            act(0)

        def step(k, carry):
            act(k)
            return carry

        lax.fori_loop(1, 64, step, 0, unroll=7)

    weights = ((k1_hbm, k1), (k2_hbm, k2), (pin_hbm, pin), (bm_hbm, bmix), (gm_hbm, gmix), (pout_hbm, pout))

    def weight(i, l):
        src, dst = weights[i]
        return pltpu.make_async_copy(src.at[l], dst.at[l], w_sem.at[l, i])

    load_image = pltpu.make_async_copy(image, cur, im_sem.at[0])
    load_image.start()
    for l in range(LAYERS):
        for i in range(len(weights)):
            weight(i, l).start()

    barrier = pltpu.get_barrier_semaphore()

    for kappa in range(2):

        def greet(k):
            r2, c2 = peer(k)
            pl.semaphore_signal(barrier, inc=1, device_id=(r2 * 2 + kappa, c2), device_id_type=MESH)

        to_group(kappa, greet)

    load_image.wait()
    zero_row = jnp.zeros((1, C), F32)

    def norm_rows(c, v, gain):
        n = norm(v, gain)
        for r in range(4):
            y = n[r * CW : (r + 1) * CW]
            i = c * 4 + r
            put_row(X, i + 2, y, zero_row, zero_row)
            for slot, j in enumerate((0, 1, CW - 2, CW - 1)):
                CBF[slot, pl.ds(i + 16, 1), :] = y[j : j + 1]

    def first_norm(c, carry):
        v = cur[pl.ds(pl.multiple_of(c * 256, 256), 256), :].astype(F32)
        norm_rows(c, v, gains[0, 0:1, :])
        return carry

    lax.fori_loop(0, CH // 4, first_norm, 0, unroll=2)

    def layer(l, carry):
        gain1 = gains[l, 1:2, :]
        CB[...] = CBF[:, 16:64, :].astype(BF16)

        @pl.when(l == 0)
        def _():
            pl.semaphore_wait(barrier, CELLS - 1)

        up, down = (row + NROW - 1) % NROW, (row + 1) % NROW
        left, right = (col + NCOL - 1) % NCOL, (col + 1) % NCOL
        plan = (
            (X.at[2 * CW : 4 * CW, C : 2 * C], HV.at[l, 1], up, col),
            (X.at[CH * CW : (CH + 2) * CW, C : 2 * C], HV.at[l, 0], down, col),
            (CB.at[0:2], HC.at[l, 1, :, 16:64], row, left),
            (CB.at[2:4], HC.at[l, 0, :, 16:64], row, right),
            (CB.at[0:2, 0:16], HC.at[l, 1, :, 64:80], up, left),
            (CB.at[2:4, 0:16], HC.at[l, 0, :, 64:80], up, right),
            (CB.at[0:2, 32:48], HC.at[l, 1, :, 0:16], down, left),
            (CB.at[2:4, 32:48], HC.at[l, 0, :, 0:16], down, right),
        )
        halo = [
            pltpu.make_async_remote_copy(
                src_ref=src, dst_ref=dst, send_sem=hs_sem.at[l, i], recv_sem=hr_sem.at[l, i],
                device_id=(r, c), device_id_type=MESH,
            )
            for i, (src, dst, r, c) in enumerate(plan)
        ]
        for copy in halo:
            copy.start()
        def conv1_dot(c, acc):
            base = c * 5
            lhs = jnp.concatenate(
                [X[pl.ds(pl.multiple_of((base + a) * CW, CW), 5 * CW), :] for a in range(3)], axis=1
            )
            acc[...] = jnp.dot(lhs, k1[l], preferred_element_type=F32)

        def conv1_rows(c, acc, edges):
            for r in range(5):
                t = c * 5 + r
                y = gelu(acc[r * CW : (r + 1) * CW, :])
                if t in (0, CH + 1):
                    y = jnp.where((row == 0) if t == 0 else (row == NROW - 1), 0.0, y)
                if edges:
                    y = jnp.where(j64 == 0, RF[1, t : t + 1, :], jnp.where(j64 == CW - 1, RF[2, t : t + 1, :], y))
                    put_row(F, t, y, RF[0, t : t + 1, :], RF[3, t : t + 1, :])
                else:
                    put_row(F, t, y, zero_row, zero_row)

        def conv1(chunks, edges):
            conv1_dot(chunks[0], A0)
            for i, c in enumerate(chunks):
                if c + 1 in chunks:
                    conv1_dot(c + 1, (A1, A0)[i % 2])
                conv1_rows(c, (A0, A1)[i % 2], edges)

        def patch(t, carry):
            base = pl.multiple_of(t * CW, CW)
            edge = [RF[k, pl.ds(t, 1), :] for k in range(4)]
            lo, hi = pl.ds(base, 16), pl.ds(base + CW - 16, 16)
            for at, lanes, fixes in (
                (lo, slice(0, C), ((0, 0), (1, 1))),
                (lo, slice(C, 2 * C), ((0, 1),)),
                (hi, slice(C, 2 * C), ((15, 2),)),
                (hi, slice(2 * C, 3 * C), ((14, 2), (15, 3))),
            ):
                v = F[at, lanes].astype(F32)
                for place, k in fixes:
                    v = jnp.where(s16 == place, edge[k], v)
                F[at, lanes] = v.astype(BF16)
            return carry

        s16 = lax.broadcasted_iota(jnp.int32, (16, C), 0)
        j64 = lax.broadcasted_iota(jnp.int32, (CW, C), 0)
        weight(0, l).wait()

        conv1(range(1, 6), False)
        for copy in halo:
            copy.wait()

        t80 = lax.broadcasted_iota(jnp.int32, (80, C), 0)
        outside = ((t80 < 16) & (row == 0)) | ((t80 >= 64) & (row == NROW - 1))
        for side, edge in ((0, col == 0), (1, col == NCOL - 1)):
            for k in range(2):
                HLF[side, k] = jnp.where(outside | edge, 0.0, HC[l, side, k].astype(F32))
        for u, part, edge in ((0, 0, row == 0), (1, 0, row == 0), (50, 1, row == NROW - 1), (51, 1, row == NROW - 1)):
            p = u % 2
            y = jnp.where(edge, 0.0, HV[l, part, p * CW : (p + 1) * CW, :].astype(F32))
            b = u + 14
            for slot, j in enumerate((0, 1, CW - 2, CW - 1)):
                CBF[slot, b : b + 1, :] = y[j : j + 1]
            put_row(X, u, y, zero_row, zero_row)

        columns = [HLF.at[0, 0], HLF.at[0, 1]] + [CBF.at[k] for k in range(4)] + [HLF.at[1, 0], HLF.at[1, 1]]
        acc = jnp.zeros((256, C), F32)
        for a in range(3):
            part = [ref[14 + a : 78 + a, :].astype(BF16) for ref in columns]
            lhs = jnp.concatenate(
                [jnp.concatenate(part[k : k + 3], axis=1) for k in (0, 1, 4, 5)], axis=0
            )
            acc = acc + jnp.dot(lhs, k1[l, a * 768 : (a + 1) * 768, :], preferred_element_type=F32)
        rim = gelu(acc)
        off = ((j64 == 0) & (row == 0)) | ((j64 == CH + 1) & (row == NROW - 1))
        for k, edge in enumerate((col == 0, False, False, col == NCOL - 1)):
            RF[k] = jnp.where(off | edge, 0.0, rim[k * 64 : (k + 1) * 64])

        def conv2_dot(c, acc):
            lhs = jnp.concatenate(
                [F[pl.ds(pl.multiple_of((c * 4 + a) * CW, CW), 4 * CW), :] for a in range(3)], axis=1
            )
            acc[...] = jnp.dot(lhs, k2[l], preferred_element_type=F32)

        def conv2_norm(c, acc, e):
            at = pl.ds(pl.multiple_of(c * 256, 256), 256)
            m = cur[at, :].astype(F32) + acc[...]
            MS[at, :] = m
            n = norm(m, gain1).astype(BF16)
            e[...] = jnp.dot(n, pin[l], preferred_element_type=F32)

        def conv2_gelu(c, e):
            at = pl.ds(pl.multiple_of(c * 256, 256), 256)
            for h, dst in enumerate((LU, LV, GU)):
                dst[at, :] = gelu(e[:, h * H : (h + 1) * H]).astype(BF16)
            GV[l, pl.ds(pl.multiple_of(c * 32, 32), 32)] = gelu(e[:, 3 * H :]).reshape(32, 8, H).astype(BF16)

        weight(1, l).wait()
        weight(2, l).wait()
        for kappa in range(2):
            if kappa == 0:
                conv1(range(0, 1), True)
                lax.fori_loop(5, 30, patch, 0, unroll=5)
            else:
                conv1(range(6, 10), True)
            accs, es = (B0, B1), (E0, E1)
            first = 6 * kappa
            for i in range(8):
                if i < 6:
                    conv2_dot(first + i, accs[i % 2])
                if 1 <= i < 7:
                    conv2_norm(first + i - 1, accs[(i - 1) % 2], es[(i - 1) % 2])
                if i >= 2:
                    conv2_gelu(first + i - 2, es[i % 2])

            def send(k):
                r2, c2 = peer(k)
                d = kappa * 64 + r2 * NCOL + c2
                pltpu.make_async_remote_copy(
                    src_ref=GV.at[l, pl.ds(d * OCT, OCT)], dst_ref=RECV.at[l, pl.ds(me * OCT, OCT)],
                    send_sem=as_sem.at[l], recv_sem=ar_sem.at[l],
                    device_id=(r2 * 2 + kappa, c2), device_id_type=MESH,
                ).start()

            to_group(kappa, send)

        def mix():
            RECV[l, pl.ds(me * OCT, OCT)] = GV[l, pl.ds(share * OCT, OCT)]
            whole = RECV.at[l, pl.ds(0, (CELLS - 1) * OCT)]
            pltpu.make_async_copy(whole, whole, ar_sem.at[l]).wait()
            S32[...] = RECV[l].astype(F32).reshape(PIX, H)
            bias = jnp.broadcast_to(gbias[pl.ds(l, 1), :], (CELLS, CELLS)).T
            for q in range(0, SHARE, 4):
                rhs = jnp.concatenate(
                    [S32[pl.ds(q + i, CELLS, stride=SHARE), :].astype(BF16) for i in range(4)], axis=1
                )
                out = jnp.dot(gmix[l], rhs, preferred_element_type=F32)
                for i in range(4):
                    S32[pl.ds(q + i, CELLS, stride=SHARE), :] = out[:, i * H : (i + 1) * H] + bias
            MIX[l] = S32[...].reshape(CELLS * OCT, 8, H).astype(BF16)
            GMV[l, pl.ds(share * OCT, OCT)] = MIX[l, pl.ds(me * OCT, OCT)]
            for kappa in range(2):

                def back(k):
                    r2, c2 = peer(k)
                    g = (r2 * 2 + kappa) * NCOL + c2
                    pltpu.make_async_remote_copy(
                        src_ref=MIX.at[l, pl.ds(g * OCT, OCT)], dst_ref=GMV.at[l, pl.ds(share * OCT, OCT)],
                        send_sem=bs_sem.at[l], recv_sem=br_sem.at[l, core],
                        device_id=(r2 * 2 + kappa, c2), device_id_type=MESH,
                    ).start()

                to_group(kappa, back)

        weight(3, l).wait()
        weight(4, l).wait()
        weight(5, l).wait()
        pl.when(core == 0)(mix)

        lbias = jnp.broadcast_to(bbias[pl.ds(l, 1), :], (H, C)).T

        def block(s, carry):
            for half in range(2):
                cols = [slice((2 * half + i) * 16, (2 * half + i + 1) * 16) for i in range(2)]

                def rows(r, cs):
                    return pl.ds(pl.multiple_of((s * 16 + r) * CW + cs.start, 16), 16)

                rhs = jnp.concatenate(
                    [jnp.concatenate([LV[rows(r, cs), :] for r in range(16)], axis=0) for cs in cols], axis=1
                )
                lm = jnp.dot(bmix[l], rhs, preferred_element_type=F32)
                for i, cs in enumerate(cols):
                    for r in range(16):
                        part = lm[r * 16 : (r + 1) * 16, i * H : (i + 1) * H] + lbias[r * 16 : (r + 1) * 16]
                        J[rows(r, cs), 0:H] = (LU[rows(r, cs), :].astype(F32) * part).astype(BF16)
            return carry

        lax.fori_loop(0, CH // 16, block, 0)
        pl.when(core == 1)(mix)

        def finish(c):
            at = pl.ds(pl.multiple_of(c * 256, 256), 256)
            gm = GMV[l, pl.ds(pl.multiple_of(c * 32, 32), 32)].astype(F32).reshape(256, H)
            gated = (GU[at, :].astype(F32) * gm).astype(BF16)
            joined = jnp.concatenate([J[at, 0:H], gated], axis=1)
            out = jnp.dot(joined, pout[l], preferred_element_type=F32)
            done = (MS[at, :] + out).astype(BF16)
            cur[at, :] = done
            return done

        def middle(c, carry):
            norm_rows(c, finish(c).astype(F32), gains[jnp.minimum(l + 1, LAYERS - 1), 0:1, :])
            return carry

        def last(c, carry):
            finish(c)
            return carry

        for kappa in range(2):
            for own in range(2):

                @pl.when(core == own)
                def _():
                    some = GMV.at[l, pl.ds(0, (64 - (own == kappa)) * OCT)]
                    pltpu.make_async_copy(some, some, br_sem.at[l, kappa]).wait()

            @pl.when(l < LAYERS - 1)
            def _():
                lax.fori_loop(6 * kappa, 6 * kappa + 6, middle, 0, unroll=2)

            @pl.when(l == LAYERS - 1)
            def _():
                lax.fori_loop(6 * kappa, 6 * kappa + 6, last, 0, unroll=2)

        whole = GV.at[l, pl.ds(0, (CELLS - 1) * OCT)]
        pltpu.make_async_copy(whole, whole, as_sem.at[l]).wait()
        whole = MIX.at[l, pl.ds(0, (CELLS - 1) * OCT)]
        pltpu.make_async_copy(whole, whole, bs_sem.at[l]).wait()
        return carry

    lax.fori_loop(0, LAYERS, layer, 0)


def on_device(image, norm_gain, conv_first, conv_second, proj_in, block_mix, block_bias, grid_mix, grid_bias, proj_out):
    any_space = pl.BlockSpec(memory_space=pl.ANY)
    vmem = pl.BlockSpec(memory_space=pltpu.VMEM)
    V = pltpu.VMEM
    DMA = pltpu.SemaphoreType.DMA
    scratch = [
        V((LAYERS, 9 * C, C), BF16), V((LAYERS, 9 * C, C), BF16), V((LAYERS, C, 2 * C), BF16),
        V((LAYERS, C, C), BF16), V((LAYERS, CELLS, CELLS), BF16), V((LAYERS, C, C), BF16),
        V(((CH + 4) * CW, 3 * C), BF16), V(((CH + 2) * CW, 3 * C), BF16), V((PIX, C), F32),
        V((PIX, H), BF16), V((PIX, H), BF16), V((PIX, H), BF16), V((LAYERS, PIX // 8, 8, H), BF16), V((PIX, H), BF16),
        V((4, 80, C), F32), V((4, CH, C), BF16), V((LAYERS, 2, 2, 80, C), BF16), V((LAYERS, 2, 2 * CW, C), BF16),
        V((2, 2, 80, C), F32), V((4, 64, C), F32),
        V((LAYERS, PIX // 8, 8, H), BF16), V((PIX, H), F32), V((LAYERS, PIX // 8, 8, H), BF16),
        V((LAYERS, PIX // 8, 8, H), BF16),
        V((5 * CW, C), F32), V((5 * CW, C), F32), V((4 * CW, C), F32), V((4 * CW, C), F32),
        V((4 * CW, 2 * C), F32), V((4 * CW, 2 * C), F32),
        DMA((LAYERS, 6)), DMA((1,)), DMA((LAYERS, 8)), DMA((LAYERS, 8)),
        DMA((LAYERS,)), DMA((LAYERS,)), DMA((LAYERS,)), DMA((LAYERS, 2)),
    ]
    out = pl.pallas_call(
        kernel,
        out_shape=jax.ShapeDtypeStruct((PIX, C), BF16),
        in_specs=[any_space, vmem] + [any_space] * 6 + [vmem, vmem],
        out_specs=vmem,
        scratch_shapes=scratch,
        compiler_params=pltpu.CompilerParams(
            collective_id=0, has_side_effects=True, vmem_limit_bytes=62 * 2**20
        ),
    )(
        image.reshape(PIX, C), norm_gain,
        conv_first.reshape(LAYERS, 9 * C, C), conv_second.reshape(LAYERS, 9 * C, C),
        proj_in, block_mix, grid_mix, proj_out, block_bias, grid_bias,
    )
    return out.reshape(image.shape)


def solution(mesh):
    placed = (P("row", "col", None), P(), P(), P(), P(), P(), P(), P(), P(), P())
    return jax.shard_map(
        on_device, mesh=mesh, in_specs=placed, out_specs=P("row", "col", None), check_vma=False
    )
```

```python
import functools

import jax
import jax.numpy as jnp
from jax import lax
from jax.experimental import pallas as pl
from jax.experimental.pallas import tpu as pltpu
from jax.sharding import PartitionSpec as P

MESH = pl.DeviceIdType.MESH
F32 = jnp.float32
BF16 = jnp.bfloat16
LAYERS = 2
CH, CW, C, H = 48, 64, 256, 128
PIX = CH * CW
NROW, NCOL, CELLS = 16, 8, 128
SHARE = PIX // CELLS
OCT = SHARE // 8
EPS = 1e-06
GA = 0.7978845608028654
GB = GA * 0.044715


def gelu(v):
    h = 0.5 * v
    return h + h * jnp.tanh(v * (GA + GB * (v * v)))


def norm(v, gain):
    mean = jnp.sum(v, axis=-1, keepdims=True) * (1.0 / C)
    centred = v - mean
    var = jnp.sum(centred * centred, axis=-1, keepdims=True) * (1.0 / C)
    return centred * lax.rsqrt(var + EPS) * gain


def put_row(dst, u, y, left, right):
    at = pl.ds(pl.multiple_of(u * CW, CW), CW)
    j = lax.broadcasted_iota(jnp.int32, (CW, C), 0)
    dst[at, 0:C] = jnp.where(j == 0, left, pltpu.roll(y, 1, 0)).astype(BF16)
    dst[at, C : 2 * C] = y.astype(BF16)
    dst[at, 2 * C : 3 * C] = jnp.where(j == CW - 1, right, pltpu.roll(y, CW - 1, 0)).astype(BF16)


def kernel(
    image, gains_hbm, k1_hbm, k2_hbm, pin_hbm, bm_hbm, gm_hbm, pout_hbm, bbias_hbm, gbias_hbm,
    result,
    cur, gains, bbias, gbias,
    k1, k2, pin, bmix, gmix, pout,
    X, F, MS, LU, LV, GU, GV, J, CBF, CB, HC, HV, HLF, RF, RECV, S32, MIX, GMV, A0, A1, B0, B1, E0, E1,
    w_sem, im_sem, out_sem, hs_sem, hr_sem, as_sem, ar_sem, bs_sem, br_sem,
):
    row, col = lax.axis_index("row"), lax.axis_index("col")
    core = row % 2
    me = row * NCOL + col
    chip = (row // 2) * NCOL + col
    share = core * 64 + chip
    half_row = lax.div(row, 2)
    columns_from = [lax.rem(col + j, NCOL) for j in range(NCOL)]

    def to_group(kappa, act):
        def step(o, carry):
            for j in range(NCOL):
                r2 = lax.rem(half_row + o + j, 8)
                if j == 0:
                    pl.when((o != 0) | (core != kappa))(functools.partial(act, r2, columns_from[j]))
                else:
                    act(r2, columns_from[j])
            return carry

        lax.fori_loop(0, 8, step, 0)

    weights = ((k1_hbm, k1), (k2_hbm, k2), (pin_hbm, pin), (bm_hbm, bmix), (gm_hbm, gmix), (pout_hbm, pout))

    def weight(i, l):
        src, dst = weights[i]
        return pltpu.make_async_copy(src.at[l], dst.at[l], w_sem.at[l, i])

    load_image = pltpu.make_async_copy(image, cur, im_sem.at[0])
    load_image.start()
    small = [
        pltpu.make_async_copy(src, dst, im_sem.at[1 + i])
        for i, (src, dst) in enumerate(((gains_hbm, gains), (bbias_hbm, bbias), (gbias_hbm, gbias)))
    ]
    for copy in small:
        copy.start()
    for l in range(LAYERS):
        for i in range(len(weights)):
            weight(i, l).start()

    barrier = pltpu.get_barrier_semaphore()

    for kappa in range(2):

        def greet(r2, c2):
            pl.semaphore_signal(barrier, inc=1, device_id=(r2 * 2 + kappa, c2), device_id_type=MESH)

        to_group(kappa, greet)

    load_image.wait()
    for copy in small:
        copy.wait()
    zero_row = jnp.zeros((1, C), F32)

    def norm_rows(c, v, gain):
        n = norm(v, gain)
        for r in range(4):
            y = n[r * CW : (r + 1) * CW]
            i = c * 4 + r
            put_row(X, i + 2, y, zero_row, zero_row)
            for slot, j in enumerate((0, 1, CW - 2, CW - 1)):
                CBF[slot, pl.ds(i + 16, 1), :] = y[j : j + 1]

    def first_norm(c, carry):
        v = cur[pl.ds(pl.multiple_of(c * 256, 256), 256), :].astype(F32)
        norm_rows(c, v, gains[0, 0:1, :])
        return carry

    lax.fori_loop(0, CH // 4, first_norm, 0, unroll=2)

    def layer(l, carry):
        gain1 = gains[l, 1:2, :]
        CB[...] = CBF[:, 16:64, :].astype(BF16)

        @pl.when(l == 0)
        def _():
            pl.semaphore_wait(barrier, CELLS - 1)

        up, down = (row + NROW - 1) % NROW, (row + 1) % NROW
        left, right = (col + NCOL - 1) % NCOL, (col + 1) % NCOL
        plan = (
            (X.at[2 * CW : 4 * CW, C : 2 * C], HV.at[l, 1], up, col),
            (X.at[CH * CW : (CH + 2) * CW, C : 2 * C], HV.at[l, 0], down, col),
            (CB.at[0:2], HC.at[l, 1, :, 16:64], row, left),
            (CB.at[2:4], HC.at[l, 0, :, 16:64], row, right),
            (CB.at[0:2, 0:16], HC.at[l, 1, :, 64:80], up, left),
            (CB.at[2:4, 0:16], HC.at[l, 0, :, 64:80], up, right),
            (CB.at[0:2, 32:48], HC.at[l, 1, :, 0:16], down, left),
            (CB.at[2:4, 32:48], HC.at[l, 0, :, 0:16], down, right),
        )
        halo = [
            pltpu.make_async_remote_copy(
                src_ref=src, dst_ref=dst, send_sem=hs_sem.at[l, i], recv_sem=hr_sem.at[l, i],
                device_id=(r, c), device_id_type=MESH,
            )
            for i, (src, dst, r, c) in enumerate(plan)
        ]
        for copy in halo:
            copy.start()
        def conv1_dot(c, acc):
            base = c * 5
            lhs = jnp.concatenate(
                [X[pl.ds(pl.multiple_of((base + a) * CW, CW), 5 * CW), :] for a in range(3)], axis=1
            )
            acc[...] = jnp.dot(lhs, k1[l], preferred_element_type=F32)

        def conv1_rows(c, acc, edges):
            for r in range(5):
                t = c * 5 + r
                y = gelu(acc[r * CW : (r + 1) * CW, :])
                if t in (0, CH + 1):
                    y = jnp.where((row == 0) if t == 0 else (row == NROW - 1), 0.0, y)
                if edges:
                    y = jnp.where(j64 == 0, RF[1, t : t + 1, :], jnp.where(j64 == CW - 1, RF[2, t : t + 1, :], y))
                    put_row(F, t, y, RF[0, t : t + 1, :], RF[3, t : t + 1, :])
                else:
                    put_row(F, t, y, zero_row, zero_row)

        def conv1(chunks, edges):
            conv1_dot(chunks[0], A0)
            for i, c in enumerate(chunks):
                if c + 1 in chunks:
                    conv1_dot(c + 1, (A1, A0)[i % 2])
                conv1_rows(c, (A0, A1)[i % 2], edges)

        def patch(t, carry):
            base = pl.multiple_of(t * CW, CW)
            edge = [RF[k, pl.ds(t, 1), :] for k in range(4)]
            lo, hi = pl.ds(base, 16), pl.ds(base + CW - 16, 16)
            for at, lanes, fixes in (
                (lo, slice(0, C), ((0, 0), (1, 1))),
                (lo, slice(C, 2 * C), ((0, 1),)),
                (hi, slice(C, 2 * C), ((15, 2),)),
                (hi, slice(2 * C, 3 * C), ((14, 2), (15, 3))),
            ):
                v = F[at, lanes].astype(F32)
                for place, k in fixes:
                    v = jnp.where(s16 == place, edge[k], v)
                F[at, lanes] = v.astype(BF16)
            return carry

        s16 = lax.broadcasted_iota(jnp.int32, (16, C), 0)
        j64 = lax.broadcasted_iota(jnp.int32, (CW, C), 0)
        weight(0, l).wait()

        conv1(range(1, 6), False)
        for copy in halo:
            copy.wait()

        t80 = lax.broadcasted_iota(jnp.int32, (80, C), 0)
        outside = ((t80 < 16) & (row == 0)) | ((t80 >= 64) & (row == NROW - 1))
        for side, edge in ((0, col == 0), (1, col == NCOL - 1)):
            for k in range(2):
                HLF[side, k] = jnp.where(outside | edge, 0.0, HC[l, side, k].astype(F32))
        for u, part, edge in ((0, 0, row == 0), (1, 0, row == 0), (50, 1, row == NROW - 1), (51, 1, row == NROW - 1)):
            p = u % 2
            y = jnp.where(edge, 0.0, HV[l, part, p * CW : (p + 1) * CW, :].astype(F32))
            b = u + 14
            for slot, j in enumerate((0, 1, CW - 2, CW - 1)):
                CBF[slot, b : b + 1, :] = y[j : j + 1]
            put_row(X, u, y, zero_row, zero_row)

        columns = [HLF.at[0, 0], HLF.at[0, 1]] + [CBF.at[k] for k in range(4)] + [HLF.at[1, 0], HLF.at[1, 1]]
        acc = jnp.zeros((256, C), F32)
        for a in range(3):
            part = [ref[14 + a : 78 + a, :].astype(BF16) for ref in columns]
            lhs = jnp.concatenate(
                [jnp.concatenate(part[k : k + 3], axis=1) for k in (0, 1, 4, 5)], axis=0
            )
            acc = acc + jnp.dot(lhs, k1[l, a * 768 : (a + 1) * 768, :], preferred_element_type=F32)
        rim = gelu(acc)
        off = ((j64 == 0) & (row == 0)) | ((j64 == CH + 1) & (row == NROW - 1))
        for k, edge in enumerate((col == 0, False, False, col == NCOL - 1)):
            RF[k] = jnp.where(off | edge, 0.0, rim[k * 64 : (k + 1) * 64])

        def conv2_dot(c, acc):
            lhs = jnp.concatenate(
                [F[pl.ds(pl.multiple_of((c * 4 + a) * CW, CW), 4 * CW), :] for a in range(3)], axis=1
            )
            acc[...] = jnp.dot(lhs, k2[l], preferred_element_type=F32)

        def conv2_norm(c, acc, e):
            at = pl.ds(pl.multiple_of(c * 256, 256), 256)
            m = cur[at, :].astype(F32) + acc[...]
            MS[at, :] = m
            n = norm(m, gain1).astype(BF16)
            e[...] = jnp.dot(n, pin[l], preferred_element_type=F32)

        def conv2_gelu(c, e):
            at = pl.ds(pl.multiple_of(c * 256, 256), 256)
            for h, dst in enumerate((LU, LV, GU)):
                dst[at, :] = gelu(e[:, h * H : (h + 1) * H]).astype(BF16)
            GV[l, pl.ds(pl.multiple_of(c * 32, 32), 32)] = gelu(e[:, 3 * H :]).reshape(32, 8, H).astype(BF16)

        weight(1, l).wait()
        weight(2, l).wait()
        for kappa in range(2):
            if kappa == 0:
                conv1(range(0, 1), True)
                lax.fori_loop(5, 30, patch, 0, unroll=5)
            else:
                conv1(range(6, 10), True)
            accs, es = (B0, B1), (E0, E1)
            first = 6 * kappa
            for i in range(8):
                if i < 6:
                    conv2_dot(first + i, accs[i % 2])
                if 1 <= i < 7:
                    conv2_norm(first + i - 1, accs[(i - 1) % 2], es[(i - 1) % 2])
                if i >= 2:
                    conv2_gelu(first + i - 2, es[i % 2])

            def send(r2, c2):
                d = kappa * 64 + r2 * NCOL + c2
                pltpu.make_async_remote_copy(
                    src_ref=GV.at[l, pl.ds(d * OCT, OCT)], dst_ref=RECV.at[l, pl.ds(me * OCT, OCT)],
                    send_sem=as_sem.at[l], recv_sem=ar_sem.at[l],
                    device_id=(r2 * 2 + kappa, c2), device_id_type=MESH,
                ).start()

            to_group(kappa, send)

        def mix():
            RECV[l, pl.ds(me * OCT, OCT)] = GV[l, pl.ds(share * OCT, OCT)]
            whole = RECV.at[l, pl.ds(0, (CELLS - 1) * OCT)]
            pltpu.make_async_copy(whole, whole, ar_sem.at[l]).wait()
            S32[...] = RECV[l].astype(F32).reshape(PIX, H)
            bias = jnp.broadcast_to(gbias[pl.ds(l, 1), :], (CELLS, CELLS)).T
            for q in range(0, SHARE, 4):
                rhs = jnp.concatenate(
                    [S32[pl.ds(q + i, CELLS, stride=SHARE), :].astype(BF16) for i in range(4)], axis=1
                )
                out = jnp.dot(gmix[l], rhs, preferred_element_type=F32)
                for i in range(4):
                    S32[pl.ds(q + i, CELLS, stride=SHARE), :] = out[:, i * H : (i + 1) * H] + bias
            MIX[l] = S32[...].reshape(CELLS * OCT, 8, H).astype(BF16)
            GMV[l, pl.ds(share * OCT, OCT)] = MIX[l, pl.ds(me * OCT, OCT)]
            for kappa in range(2):

                def back(r2, c2):
                    g = (r2 * 2 + kappa) * NCOL + c2
                    pltpu.make_async_remote_copy(
                        src_ref=MIX.at[l, pl.ds(g * OCT, OCT)], dst_ref=GMV.at[l, pl.ds(share * OCT, OCT)],
                        send_sem=bs_sem.at[l], recv_sem=br_sem.at[l, core],
                        device_id=(r2 * 2 + kappa, c2), device_id_type=MESH,
                    ).start()

                to_group(kappa, back)

        weight(3, l).wait()
        weight(4, l).wait()
        weight(5, l).wait()
        pl.when(core == 0)(mix)

        lbias = jnp.broadcast_to(bbias[pl.ds(l, 1), :], (H, C)).T

        def block(s, carry):
            for half in range(2):
                cols = [slice((2 * half + i) * 16, (2 * half + i + 1) * 16) for i in range(2)]

                def rows(r, cs):
                    return pl.ds(pl.multiple_of((s * 16 + r) * CW + cs.start, 16), 16)

                rhs = jnp.concatenate(
                    [jnp.concatenate([LV[rows(r, cs), :] for r in range(16)], axis=0) for cs in cols], axis=1
                )
                lm = jnp.dot(bmix[l], rhs, preferred_element_type=F32)
                for i, cs in enumerate(cols):
                    for r in range(16):
                        part = lm[r * 16 : (r + 1) * 16, i * H : (i + 1) * H] + lbias[r * 16 : (r + 1) * 16]
                        J[rows(r, cs), 0:H] = (LU[rows(r, cs), :].astype(F32) * part).astype(BF16)
            return carry

        lax.fori_loop(0, CH // 16, block, 0)
        pl.when(core == 1)(mix)

        def finish(c):
            at = pl.ds(pl.multiple_of(c * 256, 256), 256)
            gm = GMV[l, pl.ds(pl.multiple_of(c * 32, 32), 32)].astype(F32).reshape(256, H)
            gated = (GU[at, :].astype(F32) * gm).astype(BF16)
            joined = jnp.concatenate([J[at, 0:H], gated], axis=1)
            out = jnp.dot(joined, pout[l], preferred_element_type=F32)
            done = (MS[at, :] + out).astype(BF16)
            cur[at, :] = done
            return done

        def middle(c, carry):
            norm_rows(c, finish(c).astype(F32), gains[jnp.minimum(l + 1, LAYERS - 1), 0:1, :])
            return carry

        def last(c, carry):
            finish(c)
            return carry

        for kappa in range(2):
            for own in range(2):

                @pl.when(core == own)
                def _():
                    some = GMV.at[l, pl.ds(0, (64 - (own == kappa)) * OCT)]
                    pltpu.make_async_copy(some, some, br_sem.at[l, kappa]).wait()

            @pl.when(l < LAYERS - 1)
            def _():
                lax.fori_loop(6 * kappa, 6 * kappa + 6, middle, 0, unroll=2)

            @pl.when(l == LAYERS - 1)
            def _():
                lax.fori_loop(6 * kappa, 6 * kappa + 6, last, 0, unroll=2)
                store(kappa).start()

        whole = GV.at[l, pl.ds(0, (CELLS - 1) * OCT)]
        pltpu.make_async_copy(whole, whole, as_sem.at[l]).wait()
        whole = MIX.at[l, pl.ds(0, (CELLS - 1) * OCT)]
        pltpu.make_async_copy(whole, whole, bs_sem.at[l]).wait()
        return carry

    def store(kappa):
        half = pl.ds(kappa * (PIX // 2), PIX // 2)
        return pltpu.make_async_copy(cur.at[half], result.at[half], out_sem.at[kappa])

    lax.fori_loop(0, LAYERS, layer, 0)
    for kappa in range(2):
        store(kappa).wait()


def on_device(image, norm_gain, conv_first, conv_second, proj_in, block_mix, block_bias, grid_mix, grid_bias, proj_out):
    any_space = pl.BlockSpec(memory_space=pl.ANY)
    V = pltpu.VMEM
    DMA = pltpu.SemaphoreType.DMA
    scratch = [
        V((PIX, C), BF16), V((LAYERS, 2, C), F32), V((LAYERS, C), F32), V((LAYERS, CELLS), F32),
        V((LAYERS, 9 * C, C), BF16), V((LAYERS, 9 * C, C), BF16), V((LAYERS, C, 2 * C), BF16),
        V((LAYERS, C, C), BF16), V((LAYERS, CELLS, CELLS), BF16), V((LAYERS, C, C), BF16),
        V(((CH + 4) * CW, 3 * C), BF16), V(((CH + 2) * CW, 3 * C), BF16), V((PIX, C), F32),
        V((PIX, H), BF16), V((PIX, H), BF16), V((PIX, H), BF16), V((LAYERS, PIX // 8, 8, H), BF16), V((PIX, H), BF16),
        V((4, 80, C), F32), V((4, CH, C), BF16), V((LAYERS, 2, 2, 80, C), BF16), V((LAYERS, 2, 2 * CW, C), BF16),
        V((2, 2, 80, C), F32), V((4, 64, C), F32),
        V((LAYERS, PIX // 8, 8, H), BF16), V((PIX, H), F32), V((LAYERS, PIX // 8, 8, H), BF16),
        V((LAYERS, PIX // 8, 8, H), BF16),
        V((5 * CW, C), F32), V((5 * CW, C), F32), V((4 * CW, C), F32), V((4 * CW, C), F32),
        V((4 * CW, 2 * C), F32), V((4 * CW, 2 * C), F32),
        DMA((LAYERS, 6)), DMA((4,)), DMA((2,)), DMA((LAYERS, 8)), DMA((LAYERS, 8)),
        DMA((LAYERS,)), DMA((LAYERS,)), DMA((LAYERS,)), DMA((LAYERS, 2)),
    ]
    out = pl.pallas_call(
        kernel,
        out_shape=jax.ShapeDtypeStruct((PIX, C), BF16),
        in_specs=[any_space] * 10,
        out_specs=any_space,
        scratch_shapes=scratch,
        compiler_params=pltpu.CompilerParams(
            collective_id=0, has_side_effects=True, vmem_limit_bytes=62 * 2**20
        ),
    )(
        image.reshape(PIX, C), norm_gain,
        conv_first.reshape(LAYERS, 9 * C, C), conv_second.reshape(LAYERS, 9 * C, C),
        proj_in, block_mix, grid_mix, proj_out, block_bias, grid_bias,
    )
    return out.reshape(image.shape)


def solution(mesh):
    placed = (P("row", "col", None), P(), P(), P(), P(), P(), P(), P(), P(), P())
    return jax.shard_map(
        on_device, mesh=mesh, in_specs=placed, out_specs=P("row", "col", None), check_vma=False
    )
```

```python
import functools

import jax
import jax.numpy as jnp
from jax import lax
from jax.experimental import pallas as pl
from jax.experimental.pallas import tpu as pltpu
from jax.sharding import PartitionSpec as P

MESH = pl.DeviceIdType.MESH
F32 = jnp.float32
BF16 = jnp.bfloat16
LAYERS = 2
CH, CW, C, H = 48, 64, 256, 128
PIX = CH * CW
NROW, NCOL, CELLS = 16, 8, 128
SHARE = PIX // CELLS
OCT = SHARE // 8
EPS = 1e-06
GA = 0.7978845608028654
GB = GA * 0.044715


def gelu(v):
    h = 0.5 * v
    return h + h * jnp.tanh(v * (GA + GB * (v * v)))


def norm(v, gain):
    mean = jnp.sum(v, axis=-1, keepdims=True) * (1.0 / C)
    centred = v - mean
    var = jnp.sum(centred * centred, axis=-1, keepdims=True) * (1.0 / C)
    return centred * lax.rsqrt(var + EPS) * gain


def put_row(dst, u, y, left, right):
    at = pl.ds(pl.multiple_of(u * CW, CW), CW)
    j = lax.broadcasted_iota(jnp.int32, (CW, C), 0)
    dst[at, 0:C] = jnp.where(j == 0, left, pltpu.roll(y, 1, 0)).astype(BF16)
    dst[at, C : 2 * C] = y.astype(BF16)
    dst[at, 2 * C : 3 * C] = jnp.where(j == CW - 1, right, pltpu.roll(y, CW - 1, 0)).astype(BF16)


def kernel(
    image, gains_hbm, k1_hbm, k2_hbm, pin_hbm, bm_hbm, gm_hbm, pout_hbm, bbias_hbm, gbias_hbm,
    result,
    cur, gains, bbias, gbias,
    k1, k2, pin, bmix, gmix, pout,
    X, F, MS, LU, LV, GU, GV, J, CBF, CB, HC, HV, HLF, RF, RECV, S32, MIX, GMV, A0, A1, B0, B1, E0, E1,
    w_sem, im_sem, out_sem, hs_sem, hr_sem, as_sem, ar_sem, bs_sem, br_sem,
):
    row, col = lax.axis_index("row"), lax.axis_index("col")
    core = row % 2
    me = row * NCOL + col
    chip = (row // 2) * NCOL + col
    share = core * 64 + chip
    half_row = lax.div(row, 2)
    columns_from = [lax.rem(col + j, NCOL) for j in range(NCOL)]

    def to_group(kappa, act):
        def step(o, carry):
            for j in range(NCOL):
                r2 = lax.rem(half_row + o + j, 8)
                if j == 0:
                    pl.when((o != 0) | (core != kappa))(functools.partial(act, r2, columns_from[j]))
                else:
                    act(r2, columns_from[j])
            return carry

        lax.fori_loop(0, 8, step, 0)

    weights = ((k1_hbm, k1), (k2_hbm, k2), (pin_hbm, pin), (bm_hbm, bmix), (gm_hbm, gmix), (pout_hbm, pout))

    def weight(i, l):
        src, dst = weights[i]
        return pltpu.make_async_copy(src.at[l], dst.at[l], w_sem.at[l, i])

    load_image = pltpu.make_async_copy(image, cur, im_sem.at[0])
    load_image.start()
    small = [
        pltpu.make_async_copy(src, dst, im_sem.at[1 + i])
        for i, (src, dst) in enumerate(((gains_hbm, gains), (bbias_hbm, bbias), (gbias_hbm, gbias)))
    ]
    for copy in small:
        copy.start()
    for i in range(len(weights)):
        weight(i, 0).start()

    barrier = pltpu.get_barrier_semaphore()

    for kappa in range(2):

        def greet(r2, c2):
            pl.semaphore_signal(barrier, inc=1, device_id=(r2 * 2 + kappa, c2), device_id_type=MESH)

        to_group(kappa, greet)

    load_image.wait()
    for copy in small:
        copy.wait()
    zero_row = jnp.zeros((1, C), F32)

    def norm_rows(c, v, gain):
        n = norm(v, gain)
        for r in range(4):
            y = n[r * CW : (r + 1) * CW]
            i = c * 4 + r
            put_row(X, i + 2, y, zero_row, zero_row)
            for slot, j in enumerate((0, 1, CW - 2, CW - 1)):
                CBF[slot, pl.ds(i + 16, 1), :] = y[j : j + 1]

    def first_norm(c, carry):
        v = cur[pl.ds(pl.multiple_of(c * 256, 256), 256), :].astype(F32)
        norm_rows(c, v, gains[0, 0:1, :])
        return carry

    lax.fori_loop(0, CH // 4, first_norm, 0, unroll=3)
    for l in range(1, LAYERS):
        for i in range(len(weights)):
            weight(i, l).start()

    def layer(l, carry):
        gain1 = gains[l, 1:2, :]
        CB[...] = CBF[:, 16:64, :].astype(BF16)

        @pl.when(l == 0)
        def _():
            pl.semaphore_wait(barrier, CELLS - 1)

        up, down = (row + NROW - 1) % NROW, (row + 1) % NROW
        left, right = (col + NCOL - 1) % NCOL, (col + 1) % NCOL
        plan = (
            (X.at[2 * CW : 4 * CW, C : 2 * C], HV.at[l, 1], up, col),
            (X.at[CH * CW : (CH + 2) * CW, C : 2 * C], HV.at[l, 0], down, col),
            (CB.at[0:2], HC.at[l, 1, :, 16:64], row, left),
            (CB.at[2:4], HC.at[l, 0, :, 16:64], row, right),
            (CB.at[0:2, 0:16], HC.at[l, 1, :, 64:80], up, left),
            (CB.at[2:4, 0:16], HC.at[l, 0, :, 64:80], up, right),
            (CB.at[0:2, 32:48], HC.at[l, 1, :, 0:16], down, left),
            (CB.at[2:4, 32:48], HC.at[l, 0, :, 0:16], down, right),
        )
        halo = [
            pltpu.make_async_remote_copy(
                src_ref=src, dst_ref=dst, send_sem=hs_sem.at[l, i], recv_sem=hr_sem.at[l, i],
                device_id=(r, c), device_id_type=MESH,
            )
            for i, (src, dst, r, c) in enumerate(plan)
        ]
        for copy in halo:
            copy.start()
        def conv1_dot(c, acc):
            base = c * 5
            lhs = jnp.concatenate(
                [X[pl.ds(pl.multiple_of((base + a) * CW, CW), 5 * CW), :] for a in range(3)], axis=1
            )
            acc[...] = jnp.dot(lhs, k1[l], preferred_element_type=F32)

        def conv1_rows(c, acc, edges):
            for r in range(5):
                t = c * 5 + r
                y = gelu(acc[r * CW : (r + 1) * CW, :])
                if t in (0, CH + 1):
                    y = jnp.where((row == 0) if t == 0 else (row == NROW - 1), 0.0, y)
                if edges:
                    y = jnp.where(j64 == 0, RF[1, t : t + 1, :], jnp.where(j64 == CW - 1, RF[2, t : t + 1, :], y))
                    put_row(F, t, y, RF[0, t : t + 1, :], RF[3, t : t + 1, :])
                else:
                    put_row(F, t, y, zero_row, zero_row)

        def conv1(chunks, edges):
            conv1_dot(chunks[0], A0)
            for i, c in enumerate(chunks):
                if c + 1 in chunks:
                    conv1_dot(c + 1, (A1, A0)[i % 2])
                conv1_rows(c, (A0, A1)[i % 2], edges)

        def patch(t, carry):
            base = pl.multiple_of(t * CW, CW)
            edge = [RF[k, pl.ds(t, 1), :] for k in range(4)]
            lo, hi = pl.ds(base, 16), pl.ds(base + CW - 16, 16)
            for at, lanes, fixes in (
                (lo, slice(0, C), ((0, 0), (1, 1))),
                (lo, slice(C, 2 * C), ((0, 1),)),
                (hi, slice(C, 2 * C), ((15, 2),)),
                (hi, slice(2 * C, 3 * C), ((14, 2), (15, 3))),
            ):
                v = F[at, lanes].astype(F32)
                for place, k in fixes:
                    v = jnp.where(s16 == place, edge[k], v)
                F[at, lanes] = v.astype(BF16)
            return carry

        s16 = lax.broadcasted_iota(jnp.int32, (16, C), 0)
        j64 = lax.broadcasted_iota(jnp.int32, (CW, C), 0)
        weight(0, l).wait()

        conv1(range(1, 6), False)
        for copy in halo:
            copy.wait()

        t80 = lax.broadcasted_iota(jnp.int32, (80, C), 0)
        outside = ((t80 < 16) & (row == 0)) | ((t80 >= 64) & (row == NROW - 1))
        for side, edge in ((0, col == 0), (1, col == NCOL - 1)):
            for k in range(2):
                HLF[side, k] = jnp.where(outside | edge, 0.0, HC[l, side, k].astype(F32))
        for u, part, edge in ((0, 0, row == 0), (1, 0, row == 0), (50, 1, row == NROW - 1), (51, 1, row == NROW - 1)):
            p = u % 2
            y = jnp.where(edge, 0.0, HV[l, part, p * CW : (p + 1) * CW, :].astype(F32))
            b = u + 14
            for slot, j in enumerate((0, 1, CW - 2, CW - 1)):
                CBF[slot, b : b + 1, :] = y[j : j + 1]
            put_row(X, u, y, zero_row, zero_row)

        columns = [HLF.at[0, 0], HLF.at[0, 1]] + [CBF.at[k] for k in range(4)] + [HLF.at[1, 0], HLF.at[1, 1]]
        acc = jnp.zeros((256, C), F32)
        for a in range(3):
            part = [ref[14 + a : 78 + a, :].astype(BF16) for ref in columns]
            lhs = jnp.concatenate(
                [jnp.concatenate(part[k : k + 3], axis=1) for k in (0, 1, 4, 5)], axis=0
            )
            acc = acc + jnp.dot(lhs, k1[l, a * 768 : (a + 1) * 768, :], preferred_element_type=F32)
        rim = gelu(acc)
        off = ((j64 == 0) & (row == 0)) | ((j64 == CH + 1) & (row == NROW - 1))
        for k, edge in enumerate((col == 0, False, False, col == NCOL - 1)):
            RF[k] = jnp.where(off | edge, 0.0, rim[k * 64 : (k + 1) * 64])

        def conv2_dot(c, acc):
            lhs = jnp.concatenate(
                [F[pl.ds(pl.multiple_of((c * 4 + a) * CW, CW), 4 * CW), :] for a in range(3)], axis=1
            )
            acc[...] = jnp.dot(lhs, k2[l], preferred_element_type=F32)

        def conv2_norm(c, acc, e):
            at = pl.ds(pl.multiple_of(c * 256, 256), 256)
            m = cur[at, :].astype(F32) + acc[...]
            MS[at, :] = m
            n = norm(m, gain1).astype(BF16)
            e[...] = jnp.dot(n, pin[l], preferred_element_type=F32)

        def conv2_gelu(c, e):
            at = pl.ds(pl.multiple_of(c * 256, 256), 256)
            for h, dst in enumerate((LU, LV, GU)):
                dst[at, :] = gelu(e[:, h * H : (h + 1) * H]).astype(BF16)
            GV[l, pl.ds(pl.multiple_of(c * 32, 32), 32)] = gelu(e[:, 3 * H :]).reshape(32, 8, H).astype(BF16)

        weight(1, l).wait()
        weight(2, l).wait()
        for kappa in range(2):
            if kappa == 0:
                conv1(range(0, 1), True)
                lax.fori_loop(5, 30, patch, 0, unroll=5)
            else:
                conv1(range(6, 10), True)
            accs, es = (B0, B1), (E0, E1)
            first = 6 * kappa
            for i in range(8):
                if i < 6:
                    conv2_dot(first + i, accs[i % 2])
                if 1 <= i < 7:
                    conv2_norm(first + i - 1, accs[(i - 1) % 2], es[(i - 1) % 2])
                if i >= 2:
                    conv2_gelu(first + i - 2, es[i % 2])

            def send(r2, c2):
                d = kappa * 64 + r2 * NCOL + c2
                pltpu.make_async_remote_copy(
                    src_ref=GV.at[l, pl.ds(d * OCT, OCT)], dst_ref=RECV.at[l, pl.ds(me * OCT, OCT)],
                    send_sem=as_sem.at[l], recv_sem=ar_sem.at[l],
                    device_id=(r2 * 2 + kappa, c2), device_id_type=MESH,
                ).start()

            to_group(kappa, send)

        def mix():
            RECV[l, pl.ds(me * OCT, OCT)] = GV[l, pl.ds(share * OCT, OCT)]
            whole = RECV.at[l, pl.ds(0, (CELLS - 1) * OCT)]
            pltpu.make_async_copy(whole, whole, ar_sem.at[l]).wait()
            S32[...] = RECV[l].astype(F32).reshape(PIX, H)
            bias = jnp.broadcast_to(gbias[pl.ds(l, 1), :], (CELLS, CELLS)).T
            for q in range(0, SHARE, 4):
                rhs = jnp.concatenate(
                    [S32[pl.ds(q + i, CELLS, stride=SHARE), :].astype(BF16) for i in range(4)], axis=1
                )
                out = jnp.dot(gmix[l], rhs, preferred_element_type=F32)
                for i in range(4):
                    S32[pl.ds(q + i, CELLS, stride=SHARE), :] = out[:, i * H : (i + 1) * H] + bias
            MIX[l] = S32[...].reshape(CELLS * OCT, 8, H).astype(BF16)
            GMV[l, pl.ds(share * OCT, OCT)] = MIX[l, pl.ds(me * OCT, OCT)]
            for kappa in range(2):

                def back(r2, c2):
                    g = (r2 * 2 + kappa) * NCOL + c2
                    pltpu.make_async_remote_copy(
                        src_ref=MIX.at[l, pl.ds(g * OCT, OCT)], dst_ref=GMV.at[l, pl.ds(share * OCT, OCT)],
                        send_sem=bs_sem.at[l], recv_sem=br_sem.at[l, core],
                        device_id=(r2 * 2 + kappa, c2), device_id_type=MESH,
                    ).start()

                to_group(kappa, back)

        weight(3, l).wait()
        weight(4, l).wait()
        weight(5, l).wait()
        pl.when(core == 0)(mix)

        lbias = jnp.broadcast_to(bbias[pl.ds(l, 1), :], (H, C)).T

        def block(s, carry):
            for half in range(2):
                cols = [slice((2 * half + i) * 16, (2 * half + i + 1) * 16) for i in range(2)]

                def rows(r, cs):
                    return pl.ds(pl.multiple_of((s * 16 + r) * CW + cs.start, 16), 16)

                rhs = jnp.concatenate(
                    [jnp.concatenate([LV[rows(r, cs), :] for r in range(16)], axis=0) for cs in cols], axis=1
                )
                lm = jnp.dot(bmix[l], rhs, preferred_element_type=F32)
                for i, cs in enumerate(cols):
                    for r in range(16):
                        part = lm[r * 16 : (r + 1) * 16, i * H : (i + 1) * H] + lbias[r * 16 : (r + 1) * 16]
                        J[rows(r, cs), 0:H] = (LU[rows(r, cs), :].astype(F32) * part).astype(BF16)
            return carry

        lax.fori_loop(0, CH // 16, block, 0)
        pl.when(core == 1)(mix)

        def finish(c):
            at = pl.ds(pl.multiple_of(c * 256, 256), 256)
            gm = GMV[l, pl.ds(pl.multiple_of(c * 32, 32), 32)].astype(F32).reshape(256, H)
            gated = (GU[at, :].astype(F32) * gm).astype(BF16)
            joined = jnp.concatenate([J[at, 0:H], gated], axis=1)
            out = jnp.dot(joined, pout[l], preferred_element_type=F32)
            done = (MS[at, :] + out).astype(BF16)
            cur[at, :] = done
            return done

        def middle(c, carry):
            norm_rows(c, finish(c).astype(F32), gains[jnp.minimum(l + 1, LAYERS - 1), 0:1, :])
            return carry

        def last(c, carry):
            finish(c)
            return carry

        for kappa in range(2):
            for own in range(2):

                @pl.when(core == own)
                def _():
                    some = GMV.at[l, pl.ds(0, (64 - (own == kappa)) * OCT)]
                    pltpu.make_async_copy(some, some, br_sem.at[l, kappa]).wait()

            @pl.when(l < LAYERS - 1)
            def _():
                lax.fori_loop(6 * kappa, 6 * kappa + 6, middle, 0, unroll=3)

            @pl.when(l == LAYERS - 1)
            def _():
                lax.fori_loop(6 * kappa, 6 * kappa + 6, last, 0, unroll=3)
                store(kappa).start()

        whole = GV.at[l, pl.ds(0, (CELLS - 1) * OCT)]
        pltpu.make_async_copy(whole, whole, as_sem.at[l]).wait()
        whole = MIX.at[l, pl.ds(0, (CELLS - 1) * OCT)]
        pltpu.make_async_copy(whole, whole, bs_sem.at[l]).wait()
        return carry

    def store(kappa):
        half = pl.ds(kappa * (PIX // 2), PIX // 2)
        return pltpu.make_async_copy(cur.at[half], result.at[half], out_sem.at[kappa])

    lax.fori_loop(0, LAYERS, layer, 0)
    for kappa in range(2):
        store(kappa).wait()


def on_device(image, norm_gain, conv_first, conv_second, proj_in, block_mix, block_bias, grid_mix, grid_bias, proj_out):
    any_space = pl.BlockSpec(memory_space=pl.ANY)
    V = pltpu.VMEM
    DMA = pltpu.SemaphoreType.DMA
    scratch = [
        V((PIX, C), BF16), V((LAYERS, 2, C), F32), V((LAYERS, C), F32), V((LAYERS, CELLS), F32),
        V((LAYERS, 9 * C, C), BF16), V((LAYERS, 9 * C, C), BF16), V((LAYERS, C, 2 * C), BF16),
        V((LAYERS, C, C), BF16), V((LAYERS, CELLS, CELLS), BF16), V((LAYERS, C, C), BF16),
        V(((CH + 4) * CW, 3 * C), BF16), V(((CH + 2) * CW, 3 * C), BF16), V((PIX, C), F32),
        V((PIX, H), BF16), V((PIX, H), BF16), V((PIX, H), BF16), V((LAYERS, PIX // 8, 8, H), BF16), V((PIX, H), BF16),
        V((4, 80, C), F32), V((4, CH, C), BF16), V((LAYERS, 2, 2, 80, C), BF16), V((LAYERS, 2, 2 * CW, C), BF16),
        V((2, 2, 80, C), F32), V((4, 64, C), F32),
        V((LAYERS, PIX // 8, 8, H), BF16), V((PIX, H), F32), V((LAYERS, PIX // 8, 8, H), BF16),
        V((LAYERS, PIX // 8, 8, H), BF16),
        V((5 * CW, C), F32), V((5 * CW, C), F32), V((4 * CW, C), F32), V((4 * CW, C), F32),
        V((4 * CW, 2 * C), F32), V((4 * CW, 2 * C), F32),
        DMA((LAYERS, 6)), DMA((4,)), DMA((2,)), DMA((LAYERS, 8)), DMA((LAYERS, 8)),
        DMA((LAYERS,)), DMA((LAYERS,)), DMA((LAYERS,)), DMA((LAYERS, 2)),
    ]
    out = pl.pallas_call(
        kernel,
        out_shape=jax.ShapeDtypeStruct((PIX, C), BF16),
        in_specs=[any_space] * 10,
        out_specs=any_space,
        scratch_shapes=scratch,
        compiler_params=pltpu.CompilerParams(
            collective_id=0, has_side_effects=True, vmem_limit_bytes=62 * 2**20
        ),
    )(
        image.reshape(PIX, C), norm_gain,
        conv_first.reshape(LAYERS, 9 * C, C), conv_second.reshape(LAYERS, 9 * C, C),
        proj_in, block_mix, grid_mix, proj_out, block_bias, grid_bias,
    )
    return out.reshape(image.shape)


def solution(mesh):
    placed = (P("row", "col", None), P(), P(), P(), P(), P(), P(), P(), P(), P())
    return jax.shard_map(
        on_device, mesh=mesh, in_specs=placed, out_specs=P("row", "col", None), check_vma=False
    )
```
